32 devices in a mesh: gx: 4 (over x, core), gy: 4 (over z), gz: 2 (over y).
Axes of the slice: x: 2, y: 2, z: 4, core: 2. Of those that a mesh axis runs over, the one named last changes fastest.
Arguments:
- estimate: float32 [32, 64, 512], P('gz', 'gx', 'gy'), may hold values from 0.5 to 2
- measured: float32 [32, 64, 512], P('gz', 'gx', 'gy'), may hold values from 0.1 to 10
- point_spread: float32 [32, 1024], replicated, may hold values from 0.0005 to 4.01, as said below
Outputs:
- updated: float32 [32, 64, 512], P('gz', 'gx', 'gy')
- mip_x: float32 [32, 512], P('gz', 'gy')
- mip_y: float32 [32, 64], P('gz', 'gx')
- mip_z: float32 [64, 512], P('gx', ('gy', 'gz'))
The draws below stay inside these ranges and needn't reach their ends.
Inputs may be any that keep to these rules, and one draw needn't show every extreme that they name: `point_spread`: every entry is positive.
All inputs are finite; a program needn't handle non-finite values.
Results may differ from the reference program's by a relative error of at most 0.000076.
Values sent between devices are 32-bit elements; how exact they have to be, the bound alone decides.
A program may use at most 64 MiB of HBM per device.

```python
import math
import jax
import jax.numpy as jnp

KERNEL = 32
HALF = 16
NZ = 32
NX = 64
NY = 512


def draw_point_spread(key, part):
    offsets = jnp.arange(KERNEL, dtype=jnp.float32) - KERNEL // 2
    along_z = offsets[:, None, None]
    along_x = offsets[None, :, None]
    along_y = offsets[None, None, :]
    core = jnp.exp(-(along_z * along_z / 8.0 + along_x * along_x / 2.0 + along_y * along_y / 2.0))
    factor = jnp.exp(jax.random.uniform(key, (KERNEL, KERNEL, KERNEL), jnp.float32, math.log(0.25), math.log(4.0)))
    return ((core + 0.002) * factor).reshape(KERNEL, KERNEL * KERNEL)


def block_scale(stream_key, extent, split, low, top_value):
    level, own = 1.0, jax.random.fold_in(stream_key, 6)
    for dim, parts in split:
        heights = jnp.exp(jax.random.uniform(jax.random.fold_in(own, dim), (parts,), jnp.float32, low / len(split), top_value / len(split)))
        level = level * jnp.repeat(heights, extent[dim] // parts).reshape([-1 if axis == dim else 1 for axis in range(len(extent))])
    return level


def setup_inputs(seed: int = 0) -> dict:
    key_list = jax.random.split(jax.random.key(seed), 4)
    estimate = jnp.clip(jnp.exp(math.log(2.0) - 1.3862944 * jax.random.uniform(key_list[0], (NZ, NX, NY), jnp.float32) ** block_scale(key_list[0], (NZ, NX, NY), ((0, 2), (1, 4), (2, 4)), -0.2, 0.2)), 0.5, 2.0)
    measured = jnp.clip(jnp.exp(math.log(10.0) - 4.6051702 * jax.random.uniform(key_list[1], (NZ, NX, NY), jnp.float32) ** block_scale(key_list[1], (NZ, NX, NY), ((0, 2), (1, 4), (2, 4)), -0.2, 0.2)), 0.1, 10.0)
    point_spread = draw_point_spread(jax.random.fold_in(key_list[3], 71), 0)
    return dict(estimate=estimate, measured=measured, point_spread=point_spread)


def reference(estimate, measured, point_spread):
    psf_cube = point_spread.reshape(KERNEL, KERNEL, KERNEL)
    psf_norm = psf_cube / jnp.sum(psf_cube)
    shape_all = (NZ + KERNEL, NX + KERNEL, NY + KERNEL)
    kernel_grid = jnp.pad(psf_norm, ((0, NZ), (0, NX), (0, NY)))
    kernel_grid = jnp.roll(kernel_grid, (-HALF, -HALF, -HALF), axis=(0, 1, 2))
    spectrum = jnp.fft.rfftn(kernel_grid)
    blurred = jnp.fft.irfftn(jnp.fft.rfftn(estimate, s=shape_all) * spectrum, s=shape_all)[:NZ, :NX, :NY]
    ratio = measured / blurred
    correction = jnp.fft.irfftn(jnp.fft.rfftn(ratio, s=shape_all) * jnp.conj(spectrum), s=shape_all)[:NZ, :NX, :NY]
    updated = estimate * correction
    return updated, jnp.max(updated, axis=1), jnp.max(updated, axis=2), jnp.max(updated, axis=0)
```

```python
import functools
import math

import jax
import jax.numpy as jnp
import ml_dtypes
import numpy as np
from jax import lax
from jax.experimental import pallas as pl
from jax.experimental.pallas import tpu as pltpu
from jax.sharding import PartitionSpec as P

LANES = 128
UNROLL = 8
GRANT = 67043328
BF16 = jnp.bfloat16
F32 = jnp.float32


def round_up(value, step):
    return -(-value // step) * step


def angles(frequencies, positions, length):
    grid = np.mod(np.outer(frequencies, positions), length)
    return grid * (2.0 * math.pi / length)


def parts_of(table):
    high = table.astype(np.float32).astype(ml_dtypes.bfloat16)
    low = (table - high.astype(np.float64)).astype(np.float32).astype(ml_dtypes.bfloat16)
    return high, low


def left_table(frequencies, positions, length, transpose=False):
    theta = angles(frequencies, positions, length)
    if transpose:
        theta = theta.T
    high, low = parts_of(np.concatenate([np.cos(theta), np.sin(theta)], axis=0))
    return np.concatenate([high, high, low], axis=1)


def forward_rows(positions, length, bins, lanes, rows):
    theta = angles(positions, np.arange(bins), length)
    table = np.zeros((rows, 2 * lanes))
    table[: len(positions), :bins] = np.cos(theta)
    table[: len(positions), lanes : lanes + bins] = -np.sin(theta)
    return parts_of(table)


def inverse_rows(positions, length, bins, lanes, scale):
    theta = angles(np.arange(bins), positions, length)
    weight = np.full((bins, 1), 2.0)
    weight[0] = 1.0
    if length % 2 == 0:
        weight[-1] = 1.0
    table = np.zeros((2 * lanes, len(positions)))
    table[:bins] = weight * np.cos(theta) * scale
    table[lanes : lanes + bins] = -weight * np.sin(theta) * scale
    return parts_of(table)


class Plan:
    def __init__(self, brick, extent, mesh):
        self.mesh = mesh
        self.extent = extent
        self.margin = extent // 2
        self.brick_z, self.brick_x, self.brick_y = brick
        self.rows = self.brick_z * self.brick_x
        self.length_z = self.brick_z + extent
        self.length_x = self.brick_x + extent
        self.length_y = self.brick_y + extent
        self.bins = self.length_y // 2 + 1
        self.lanes = round_up(self.bins, LANES)
        self.pitch = self.length_z + 8
        self.pitch_back = self.length_x + 8
        self.pitch_psf = extent + 8
        self.groups = LANES // extent
        self.packed = self.rows // self.groups

    def tables(self):
        m = self.margin
        offsets = np.arange(self.extent) - m
        high, low = forward_rows(offsets, self.length_y, self.bins, self.lanes, self.extent)
        high, low = np.tile(high, (self.groups, 1)), np.tile(low, (self.groups, 1))
        frequency_x = np.arange(self.length_x)
        frequency_z = np.arange(self.length_z)
        psf_y = np.concatenate([high, high, low], axis=0)
        psf_x = left_table(frequency_x, offsets, self.length_x)
        psf_z = left_table(frequency_z, offsets, self.length_z)
        core = np.arange(self.brick_y) + m
        side = np.concatenate([np.arange(m), np.arange(m) + m + self.brick_y])
        core_high, core_low = forward_rows(core, self.length_y, self.bins, self.lanes, self.brick_y)
        side_high, side_low = forward_rows(side, self.length_y, self.bins, self.lanes, self.extent)
        side_high, side_low = np.tile(side_high, (self.groups, 1)), np.tile(side_low, (self.groups, 1))
        wide = np.concatenate([core_high, core_high, core_low, side_high, side_high, side_low], axis=0)
        along_x = left_table(frequency_x, frequency_x, self.length_x)
        along_z = left_table(frequency_z, frequency_z, self.length_z)
        back_z = left_table(frequency_z, np.arange(self.brick_z) + m, self.length_z, True)
        back_x = left_table(frequency_x, np.arange(self.brick_x) + m, self.length_x, True)
        scale = 1.0 / float(self.length_z * self.length_x * self.length_y)
        high, low = inverse_rows(core, self.length_y, self.bins, self.lanes, scale)
        back_y = np.concatenate([high, low], axis=1)
        return psf_y, psf_x, psf_z, wide, along_x, along_z, back_z, back_x, back_y


def split(values):
    high = values.astype(BF16)
    low = (values - high.astype(F32)).astype(BF16)
    return high, low


def dot(left, right):
    return jnp.dot(left, right, preferred_element_type=F32)


def apply_left(table, values, sign):
    lanes = values.shape[1] // 2
    high, low = split(values)
    out = dot(table, jnp.concatenate([high, low, high], axis=0))
    half = out.shape[0] // 2
    top_re, top_im = out[:half, :lanes], out[:half, lanes:]
    low_re, low_im = out[half:, :lanes], out[half:, lanes:]
    if sign < 0:
        return top_re + low_im, top_im - low_re
    return top_re - low_im, top_im + low_re


def loop(count, body, unroll):
    def step(i, carry):
        body(i)
        return carry

    lax.fori_loop(0, count, step, 0, unroll=math.gcd(count, unroll))


def aligned(value, step):
    return pl.multiple_of(value, step)


AXES = ("gz", "gx", "gy")


def lane_index(rows):
    return lax.broadcasted_iota(jnp.int32, (rows, LANES), 1)


class Exchange:
    def __init__(self, plan, number, refs, ends):
        self.plan, self.number, self.ends = plan, number, ends
        self.block, self.side, self.left, self.right, self.pack, self.send, self.recv = refs

    def copy(self, source, target, slot, axis, step):
        return pltpu.make_async_remote_copy(
            src_ref=source,
            dst_ref=target,
            send_sem=self.send.at[self.number, slot],
            recv_sem=self.recv.at[self.number, slot],
            device_id={axis: lax.axis_index(axis) + step},
            device_id_type=pl.DeviceIdType.MESH,
        )

    def pair(self, axis, source, targets, slot, guard=None, sources=None):
        low, high = self.ends[axis]
        out = []
        for k, step in ((0, 1), (1, -1)):
            sends, receives = (high, low) if step == 1 else (low, high)
            if guard is not None:
                sends, receives = jnp.logical_and(sends, guard), jnp.logical_and(receives, guard)
            piece = source if sources is None else sources[k]
            out.append((sends, receives, self.copy(piece, targets[k], slot + k, axis, step)))
        return out

    def plans(self, brick):
        e, block, side = self.number, self.block, self.side
        low, high = self.ends["gz"]
        self.y = self.pair("gy", None, (self.left.at[e], self.right.at[e]), 0, None, (self.pack.at[e, 0], self.pack.at[e, 1]))
        self.z = self.pair("gz", brick, (block.at[e, 0, 1], block.at[e, 2, 1]), 2)
        self.x = self.pair("gx", brick, (block.at[e, 1, 0], block.at[e, 1, 2]), 4)
        self.side_z = self.pair("gz", side.at[e, 1, 1], (side.at[e, 0, 1], side.at[e, 2, 1]), 6)
        self.side_x = self.pair("gx", side.at[e, 1, 1], (side.at[e, 1, 0], side.at[e, 1, 2]), 8)
        self.far_x, self.far_side = [], []
        for k, (zb, guard) in enumerate(((0, low), (2, high))):
            self.far_x.append(self.pair("gx", block.at[e, zb, 1], (block.at[e, zb, 0], block.at[e, zb, 2]), 10 + 2 * k, guard))
            self.far_side.append(self.pair("gx", side.at[e, zb, 1], (side.at[e, zb, 0], side.at[e, zb, 2]), 14 + 2 * k, guard))

    def begin(self, copies):
        for sends, _, item in copies:
            @pl.when(sends)
            def _(item=item):
                item.start()

    def arrive(self, copies):
        for _, receives, item in copies:
            @pl.when(receives)
            def _(item=item):
                item.wait_recv()

    def leave(self):
        for copies in (self.y, self.z, self.x, self.side_z, self.side_x, *self.far_x, *self.far_side):
            for sends, _, item in copies:
                @pl.when(sends)
                def _(item=item):
                    item.wait_send()

    def start(self, brick):
        plan, e = self.plan, self.number
        self.plans(brick)
        m, packed, width = plan.margin, plan.packed, plan.brick_y
        lane = lane_index(packed)
        head, tail = jnp.zeros((packed, LANES), F32), jnp.zeros((packed, LANES), F32)
        for j in range(plan.groups):
            rows = slice(j * packed, (j + 1) * packed)
            first = lane // m == 2 * j
            second = lane // m == 2 * j + 1
            tail = jnp.where(first, pltpu.roll(brick[rows, width - LANES :], (2 * j * m + m) % LANES, 1), tail)
            head = jnp.where(second, pltpu.roll(brick[rows, :LANES], (2 * j + 1) * m % LANES, 1), head)
        self.pack[e, 0] = tail
        self.pack[e, 1] = head
        self.begin(self.y)
        self.begin(self.x)
        self.begin(self.z)

    def middle(self):
        plan, e = self.plan, self.number
        self.arrive(self.y)
        lane = lane_index(plan.packed)
        self.side[e, 1, 1] = jnp.where(lane // plan.margin % 2 == 0, self.left[e], self.right[e])
        self.begin(self.side_x)
        self.begin(self.side_z)
        for k in range(2):
            self.arrive(self.z[k : k + 1])
            self.begin(self.far_x[k])

    def last(self):
        for k in range(2):
            self.arrive(self.side_z[k : k + 1])
            self.begin(self.far_side[k])


def psf_first(plan, p_ref, wy_ref, tz_ref, y_ref, sre_ref, sim_ref):
    extent = plan.extent
    total = jnp.sum(jnp.sum(p_ref[...], axis=0, keepdims=True), axis=1, keepdims=True)
    tiles = extent // plan.groups
    values = jnp.concatenate([p_ref[:, t * LANES : (t + 1) * LANES] for t in range(tiles)], axis=0)
    lane = lane_index(values.shape[0])
    for j in range(plan.groups):
        high, low = split(jnp.where(lane // extent == j, values, 0.0))
        out = dot(jnp.concatenate([high, low], axis=1), wy_ref[: 2 * LANES, :]) + dot(high, wy_ref[2 * LANES :, :])
        out = out / total
        for t in range(tiles):
            a = plan.groups * t + j
            y_ref[a * extent : (a + 1) * extent, :] = out[t * extent : (t + 1) * extent]

    def along_z(a):
        re, im = apply_left(tz_ref[...], y_ref[pl.ds(aligned(a * extent, 8), extent), :], -1)
        sre_ref[pl.ds(a, plan.length_z, stride=plan.pitch_psf), :] = re
        sim_ref[pl.ds(a, plan.length_z, stride=plan.pitch_psf), :] = im

    loop(extent, along_z, 8)


def psf_second(plan, tx_ref, sre_ref, sim_ref, kre_ref, kim_ref):
    def along_x(l):
        rows = pl.ds(aligned(l * plan.pitch_psf, 8), plan.extent)
        values = jnp.concatenate([sre_ref[rows, :], sim_ref[rows, :]], axis=1)
        re, im = apply_left(tx_ref[...], values, -1)
        kre_ref[pl.ds(l, plan.length_x, stride=plan.pitch), :] = re
        kim_ref[pl.ds(l, plan.length_x, stride=plan.pitch), :] = im

    loop(plan.length_z, along_x, 8)


def block_y(plan, values, packed, wy_ref):
    core2, wide = 2 * plan.brick_y, plan.brick_y + LANES
    core_high, core_low = split(values)
    lane = lane_index(plan.packed)
    side = jnp.concatenate([jnp.where(lane // plan.extent == j, packed, 0.0) for j in range(plan.groups)], axis=0)
    side_high, side_low = split(side)
    return (
        dot(jnp.concatenate([core_high, core_low], axis=1), wy_ref[:core2, :])
        + dot(jnp.concatenate([core_high, side_high], axis=1), wy_ref[core2 : core2 + wide, :])
        + dot(jnp.concatenate([side_low, side_high], axis=1), wy_ref[core2 + wide :, :])
    )


def transform(plan, conj, valid_z, tables, spectrum, scratch):
    tx_ref, tz_ref, bz_ref, bx_ref, by_ref = tables
    kre_ref, kim_ref = spectrum
    y_ref, sre_ref, sim_ref, ire_ref, iim_ref, f_ref = scratch
    length_z, length_x, pitch, back = plan.length_z, plan.length_x, plan.pitch, plan.pitch_back
    bz, bx = plan.brick_z, plan.brick_x

    for zb in range(3):
        @pl.when(valid_z[zb])
        def _(zb=zb):
            def along_x(z):
                rows = pl.ds(aligned(z * bx, 8), bx)
                values = jnp.concatenate([y_ref[zb, xb, rows, :] for xb in range(3)], axis=0)
                re, im = apply_left(tx_ref[...], values, -1)
                sre_ref[pl.ds(zb * bz + z, length_x, stride=pitch), :] = re
                sim_ref[pl.ds(zb * bz + z, length_x, stride=pitch), :] = im

            loop(bz, along_x, UNROLL)

    group = math.gcd(length_x, UNROLL)

    def along_z(step):
        products = []
        for i in range(group):
            k = step * group + i
            rows = pl.ds(aligned(k * pitch, 8), length_z)
            values = jnp.concatenate([sre_ref[rows, :], sim_ref[rows, :]], axis=1)
            re, im = apply_left(tz_ref[...], values, -1)
            kre, kim = kre_ref[rows, :], kim_ref[rows, :]
            if conj:
                pre, pim = re * kre + im * kim, im * kre - re * kim
            else:
                pre, pim = re * kre - im * kim, re * kim + im * kre
            products.append(jnp.concatenate([pre, pim], axis=1))
        for i in range(group):
            re, im = apply_left(bz_ref[...], products[i], 1)
            ire_ref[pl.ds(step * group + i, bz, stride=back), :] = re
            iim_ref[pl.ds(step * group + i, bz, stride=back), :] = im

    loop(length_x // group, along_z, 1)

    def back_x(z):
        rows = pl.ds(aligned(z * back, 8), length_x)
        values = jnp.concatenate([ire_ref[rows, :], iim_ref[rows, :]], axis=1)
        re, im = apply_left(bx_ref[...], values, 1)
        f_ref[pl.ds(aligned(z * bx, 8), bx), :] = jnp.concatenate([re, im], axis=1)

    loop(bz, back_x, UNROLL)
    high, low = split(f_ref[...])
    by = plan.brick_y
    both = dot(high, by_ref[...])
    return both[:, :by] + both[:, by:] + dot(low, by_ref[:, :by])


def kernel(plan, *rest):
    sources = rest[:12]
    out_ref, across_ref, along_ref, top_ref = rest[12:16]
    held = rest[16:28]
    e_ref, m_ref, p_ref, psf_y, psf_x, psf_z, wy_ref = held[:7]
    tables = held[7:]
    (block, side, left, right, pack, ratio, py_ref, pre_ref, pim_ref, kre_ref, kim_ref,
     y_ref, sre_ref, sim_ref, ire_ref, iim_ref, f_ref,
     most_z, most_x, most_y, send, recv, most_send, most_recv, fetch) = rest[28:]
    fetched = [pltpu.make_async_copy(sources[i], held[i], fetch.at[i]) for i in range(12)]
    for i in (0, 2, 3, 5, 4, 6, 1, 7, 8, 9, 10, 11):
        fetched[i].start()
    most = {"gz": most_z, "gx": most_x, "gy": most_y}
    count = plan.mesh

    barrier = pltpu.get_barrier_semaphore()
    peers = 0
    for axis in AXES:
        for d in range(1, count[axis]):
            other = (lax.axis_index(axis) + d) % count[axis]
            pl.semaphore_signal(barrier, inc=1, device_id={axis: other}, device_id_type=pl.DeviceIdType.MESH)
            peers += 1
    pl.semaphore_wait(barrier, peers)

    ends = {axis: (lax.axis_index(axis) > 0, lax.axis_index(axis) < count[axis] - 1) for axis in AXES}
    valid_z = (ends["gz"][0], ends["gz"][0] | True, ends["gz"][1])
    valid_x = (ends["gx"][0], ends["gx"][0] | True, ends["gx"][1])
    refs = (block, side, left, right, pack, send, recv)
    first, second = Exchange(plan, 0, refs, ends), Exchange(plan, 1, refs, ends)

    fetched[0].wait()
    first.start(e_ref)
    for target, has in ((left, ends["gy"][0]), (right, ends["gy"][1])):
        @pl.when(jnp.logical_not(has))
        def _(target=target):
            target[...] = jnp.zeros_like(target)
    for zb in (0, 2):
        @pl.when(jnp.logical_not(valid_z[zb]))
        def _(zb=zb):
            def clear(k):
                rows = pl.ds(aligned(k * plan.pitch + zb * plan.brick_z, 8), plan.brick_z)
                zero = jnp.zeros((plan.brick_z, plan.lanes), F32)
                sre_ref[rows, :] = zero
                sim_ref[rows, :] = zero

            loop(plan.length_x, clear, 8)
    for xb in (0, 2):
        @pl.when(jnp.logical_not(valid_x[xb]))
        def _(xb=xb):
            for zb in range(3):
                y_ref[zb, xb] = jnp.zeros((plan.rows, 2 * plan.lanes), F32)

    def along_y(exchange, zb, xb, brick):
        @pl.when(jnp.logical_and(valid_z[zb], valid_x[xb]))
        def _():
            e = exchange.number
            values = brick[...] if (zb, xb) == (1, 1) else block[e, zb, xb]
            y_ref[zb, xb] = block_y(plan, values, side[e, zb, xb], wy_ref)

    def rest_of(exchange, brick):
        along_y(exchange, 1, 1, brick)
        along_y(exchange, 0, 1, brick)
        along_y(exchange, 2, 1, brick)
        exchange.arrive(exchange.x)
        exchange.arrive(exchange.side_x)
        along_y(exchange, 1, 0, brick)
        along_y(exchange, 1, 2, brick)
        for k, zb in enumerate((0, 2)):
            exchange.arrive(exchange.far_x[k])
            exchange.arrive(exchange.far_side[k])
            along_y(exchange, zb, 0, brick)
            along_y(exchange, zb, 2, brick)

    scratch = (y_ref, sre_ref, sim_ref, ire_ref, iim_ref, f_ref)
    for i in (2, 3, 5):
        fetched[i].wait()
    psf_first(plan, p_ref, psf_y, psf_z, py_ref, pre_ref, pim_ref)
    first.middle()
    fetched[4].wait()
    psf_second(plan, psf_x, pre_ref, pim_ref, kre_ref, kim_ref)
    first.last()
    for i in (6, 1, 7, 8, 9, 10, 11):
        fetched[i].wait()
    rest_of(first, e_ref)
    blurred = transform(plan, False, valid_z, tables, (kre_ref, kim_ref), scratch)
    ratio[...] = m_ref[...] / blurred

    second.start(ratio)
    second.middle()
    second.last()
    rest_of(second, ratio)
    correction = transform(plan, True, valid_z, tables, (kre_ref, kim_ref), scratch)
    updated = (e_ref[...] * correction).reshape(plan.brick_z, plan.brick_x, plan.brick_y)
    out_ref[...] = updated

    most_x[0] = jnp.max(updated, axis=1)
    most_y[0] = jnp.zeros((plan.brick_z, LANES), F32)
    most_y[0, :, : plan.brick_x] = jnp.max(updated, axis=2)
    most_z[0] = jnp.max(updated, axis=0)
    copies = {}
    slot = 0
    for axis in AXES:
        copies[axis] = []
        for d in range(1, count[axis]):
            item = pltpu.make_async_remote_copy(
                src_ref=most[axis].at[0],
                dst_ref=most[axis].at[d],
                send_sem=most_send.at[slot],
                recv_sem=most_recv.at[slot],
                device_id={axis: (lax.axis_index(axis) + d) % count[axis]},
                device_id_type=pl.DeviceIdType.MESH,
            )
            item.start()
            copies[axis].append(item)
            slot += 1
    first.leave()
    second.leave()
    found = {}
    for axis in AXES:
        value = most[axis][0]
        for d, item in enumerate(copies[axis]):
            item.wait_recv()
            value = jnp.maximum(value, most[axis][d + 1])
        found[axis] = value
    across_ref[...] = found["gx"]
    along_ref[...] = found["gy"][:, : plan.brick_x]
    piece = plan.brick_y // count["gz"]
    for i in range(count["gz"]):
        @pl.when(lax.axis_index("gz") == i)
        def _(i=i):
            top_ref[...] = found["gz"][:, i * piece : (i + 1) * piece]
    for axis in AXES:
        for item in copies[axis]:
            item.wait_send()


def deliver(count, *refs):
    sources, targets, held, sems = refs[:count], refs[count : 2 * count], refs[2 * count : 3 * count], refs[-1]
    inward = [pltpu.make_async_copy(sources[i], held[i], sems.at[0, i]) for i in range(count)]
    outward = [pltpu.make_async_copy(held[i], targets[i], sems.at[1, i]) for i in range(count)]
    for item in inward:
        item.start()
    for i in range(count):
        inward[i].wait()
        outward[i].start()
    for item in outward:
        item.wait()


def shards(sizes, estimate, measured, point_spread):
    plan = Plan(estimate.shape, point_spread.shape[0], sizes)
    bz, bx, by, rows = plan.brick_z, plan.brick_x, plan.brick_y, plan.rows
    args = (estimate.reshape(rows, by), measured.reshape(rows, by), point_spread, *plan.tables())
    vmem = pl.BlockSpec(memory_space=pltpu.VMEM)
    outs = [(bz, bx, by), (bz, by), (bz, bx), (bx, by // sizes["gz"])]
    spread = (plan.length_x * plan.pitch, plan.lanes)
    psf_spread = (plan.length_z * plan.pitch_psf, plan.lanes)
    back = (bz * plan.pitch_back, plan.lanes)
    shapes = [
        (2, 3, 3, rows, by), (2, 3, 3, plan.packed, LANES), (2, plan.packed, LANES), (2, plan.packed, LANES),
        (2, 2, plan.packed, LANES), (rows, by), (plan.extent * plan.extent, 2 * plan.lanes), psf_spread, psf_spread,
        spread, spread, (3, 3, rows, 2 * plan.lanes), spread, spread, back, back, (rows, 2 * plan.lanes),
        (sizes["gz"], bx, by), (sizes["gx"], bz, by), (sizes["gy"], bz, LANES),
    ]
    peers = sum(sizes[axis] - 1 for axis in AXES)
    sems = pltpu.SemaphoreType.DMA
    held = [pltpu.VMEM(item.shape, item.dtype) for item in args]
    results = pl.pallas_call(
        functools.partial(kernel, plan),
        out_shape=[jax.ShapeDtypeStruct(shape, F32) for shape in outs],
        in_specs=[pl.BlockSpec(memory_space=pltpu.HBM)] * len(args),
        out_specs=[vmem] * len(outs),
        scratch_shapes=held + [pltpu.VMEM(shape, F32) for shape in shapes]
        + [sems((2, 18)), sems((2, 18)), sems((peers,)), sems((peers,)), sems((len(args),))],
        compiler_params=pltpu.CompilerParams(collective_id=0, has_side_effects=True, vmem_limit_bytes=GRANT),
    )(*args)
    return pl.pallas_call(
        functools.partial(deliver, len(outs)),
        out_shape=[jax.ShapeDtypeStruct(shape, F32) for shape in outs],
        in_specs=[pl.BlockSpec(memory_space=pltpu.HBM)] * len(outs),
        out_specs=[pl.BlockSpec(memory_space=pltpu.HBM)] * len(outs),
        scratch_shapes=[pltpu.VMEM(shape, F32) for shape in outs] + [sems((2, len(outs)))],
        compiler_params=pltpu.CompilerParams(vmem_limit_bytes=GRANT),
    )(*results)


def solution(mesh):
    in_specs = (P("gz", "gx", "gy"), P("gz", "gx", "gy"), P())
    out_specs = (P("gz", "gx", "gy"), P("gz", "gy"), P("gz", "gx"), P("gx", ("gy", "gz")))
    body = functools.partial(shards, {axis: mesh.shape[axis] for axis in AXES})
    return jax.shard_map(lambda *args: tuple(body(*args)), mesh=mesh, in_specs=in_specs, out_specs=out_specs, check_vma=False)
```

```python
import functools
import math

import jax
import jax.numpy as jnp
import ml_dtypes
import numpy as np
from jax import lax
from jax.experimental import pallas as pl
from jax.experimental.pallas import tpu as pltpu
from jax.sharding import PartitionSpec as P

LANES = 128
UNROLL = 16
GRANT = 66879488
ROOM = 1 << 20
BF16 = jnp.bfloat16
F32 = jnp.float32


def round_up(value, step):
    return -(-value // step) * step


def angles(frequencies, positions, length):
    grid = np.mod(np.outer(frequencies, positions), length)
    return grid * (2.0 * math.pi / length)


def parts_of(table):
    high = table.astype(np.float32).astype(ml_dtypes.bfloat16)
    low = (table - high.astype(np.float64)).astype(np.float32).astype(ml_dtypes.bfloat16)
    return high, low


def left_table(frequencies, positions, length, transpose=False):
    theta = angles(frequencies, positions, length)
    if transpose:
        theta = theta.T
    high, low = parts_of(np.concatenate([np.cos(theta), np.sin(theta)], axis=0))
    return np.concatenate([high, high, low], axis=1)


def forward_rows(positions, length, bins, lanes, rows):
    theta = angles(positions, np.arange(bins), length)
    table = np.zeros((rows, 2 * lanes))
    table[: len(positions), :bins] = np.cos(theta)
    table[: len(positions), lanes : lanes + bins] = -np.sin(theta)
    return parts_of(table)


def inverse_rows(positions, length, bins, lanes, scale):
    theta = angles(np.arange(bins), positions, length)
    weight = np.full((bins, 1), 2.0)
    weight[0] = 1.0
    if length % 2 == 0:
        weight[-1] = 1.0
    table = np.zeros((2 * lanes, len(positions)))
    table[:bins] = weight * np.cos(theta) * scale
    table[lanes : lanes + bins] = -weight * np.sin(theta) * scale
    return parts_of(table)


class Plan:
    def __init__(self, brick, extent, mesh):
        self.mesh = mesh
        self.extent = extent
        self.margin = extent // 2
        self.brick_z, self.brick_x, self.brick_y = brick
        self.rows = self.brick_z * self.brick_x
        self.length_z = self.brick_z + extent
        self.length_x = self.brick_x + extent
        self.length_y = self.brick_y + extent
        self.bins = self.length_y // 2 + 1
        self.lanes = round_up(self.bins, LANES)
        self.pitch = self.length_z + 8
        self.pitch_back = self.length_x + 8
        self.pitch_psf = extent + 8
        self.groups = LANES // extent
        self.packed = self.rows // self.groups

    def tables(self):
        m = self.margin
        offsets = np.arange(self.extent) - m
        high, low = forward_rows(offsets, self.length_y, self.bins, self.lanes, self.extent)
        high, low = np.tile(high, (self.groups, 1)), np.tile(low, (self.groups, 1))
        frequency_x = np.arange(self.length_x)
        frequency_z = np.arange(self.length_z)
        psf_y = np.concatenate([high, high, low], axis=0)
        psf_x = left_table(frequency_x, offsets, self.length_x)
        psf_z = left_table(frequency_z, offsets, self.length_z)
        core = np.arange(self.brick_y) + m
        side = np.concatenate([np.arange(m), np.arange(m) + m + self.brick_y])
        core_high, core_low = forward_rows(core, self.length_y, self.bins, self.lanes, self.brick_y)
        side_high, side_low = forward_rows(side, self.length_y, self.bins, self.lanes, self.extent)
        side_high, side_low = np.tile(side_high, (self.groups, 1)), np.tile(side_low, (self.groups, 1))
        wide = np.concatenate([core_high, core_high, core_low, side_high, side_high, side_low], axis=0)
        along_x = left_table(frequency_x, frequency_x, self.length_x)
        along_z = left_table(frequency_z, frequency_z, self.length_z)
        back_z = left_table(frequency_z, np.arange(self.brick_z) + m, self.length_z, True)
        back_x = left_table(frequency_x, np.arange(self.brick_x) + m, self.length_x, True)
        scale = 1.0 / float(self.length_z * self.length_x * self.length_y)
        high, low = inverse_rows(core, self.length_y, self.bins, self.lanes, scale)
        back_y = np.concatenate([high, low], axis=1)
        return psf_y, psf_x, psf_z, wide, along_x, along_z, back_z, back_x, back_y


def split(values):
    high = values.astype(BF16)
    low = (values - high.astype(F32)).astype(BF16)
    return high, low


def dot(left, right):
    return jnp.dot(left, right, preferred_element_type=F32)


def apply_left(table, values, sign):
    lanes = values.shape[1] // 2
    high, low = split(values)
    out = dot(table, jnp.concatenate([high, low, high], axis=0))
    half = out.shape[0] // 2
    top_re, top_im = out[:half, :lanes], out[:half, lanes:]
    low_re, low_im = out[half:, :lanes], out[half:, lanes:]
    if sign < 0:
        return top_re + low_im, top_im - low_re
    return top_re - low_im, top_im + low_re


def loop(count, body, unroll):
    def step(i, carry):
        body(i)
        return carry

    lax.fori_loop(0, count, step, 0, unroll=math.gcd(count, unroll))


def aligned(value, step):
    return pl.multiple_of(value, step)


AXES = ("gz", "gx", "gy")


def lane_index(rows):
    return lax.broadcasted_iota(jnp.int32, (rows, LANES), 1)


class Exchange:
    def __init__(self, plan, number, refs, ends):
        self.plan, self.number, self.ends = plan, number, ends
        self.block, self.side, self.left, self.right, self.pack, self.send, self.recv = refs

    def copy(self, source, target, slot, axis, step):
        return pltpu.make_async_remote_copy(
            src_ref=source,
            dst_ref=target,
            send_sem=self.send.at[self.number, slot],
            recv_sem=self.recv.at[self.number, slot],
            device_id={axis: lax.axis_index(axis) + step},
            device_id_type=pl.DeviceIdType.MESH,
        )

    def pair(self, axis, source, targets, slot, guard=None, sources=None):
        low, high = self.ends[axis]
        out = []
        for k, step in ((0, 1), (1, -1)):
            sends, receives = (high, low) if step == 1 else (low, high)
            if guard is not None:
                sends, receives = jnp.logical_and(sends, guard), jnp.logical_and(receives, guard)
            piece = source if sources is None else sources[k]
            out.append((sends, receives, self.copy(piece, targets[k], slot + k, axis, step)))
        return out

    def plans(self, brick):
        e, block, side = self.number, self.block, self.side
        low, high = self.ends["gz"]
        self.y = self.pair("gy", None, (self.left.at[e], self.right.at[e]), 0, None, (self.pack.at[e, 0], self.pack.at[e, 1]))
        self.z = self.pair("gz", brick, (block.at[e, 0, 1], block.at[e, 2, 1]), 2)
        self.x = self.pair("gx", brick, (block.at[e, 1, 0], block.at[e, 1, 2]), 4)
        self.side_z = self.pair("gz", side.at[e, 1, 1], (side.at[e, 0, 1], side.at[e, 2, 1]), 6)
        self.side_x = self.pair("gx", side.at[e, 1, 1], (side.at[e, 1, 0], side.at[e, 1, 2]), 8)
        self.far_x, self.far_side = [], []
        for k, (zb, guard) in enumerate(((0, low), (2, high))):
            self.far_x.append(self.pair("gx", block.at[e, zb, 1], (block.at[e, zb, 0], block.at[e, zb, 2]), 10 + 2 * k, guard))
            self.far_side.append(self.pair("gx", side.at[e, zb, 1], (side.at[e, zb, 0], side.at[e, zb, 2]), 14 + 2 * k, guard))

    def begin(self, copies):
        for sends, _, item in copies:
            @pl.when(sends)
            def _(item=item):
                item.start()

    def arrive(self, copies):
        for _, receives, item in copies:
            @pl.when(receives)
            def _(item=item):
                item.wait_recv()

    def leave(self):
        for copies in (self.y, self.z, self.x, self.side_z, self.side_x, *self.far_x, *self.far_side):
            for sends, _, item in copies:
                @pl.when(sends)
                def _(item=item):
                    item.wait_send()

    def start(self, brick):
        plan, e = self.plan, self.number
        self.plans(brick)
        m, packed, width = plan.margin, plan.packed, plan.brick_y
        lane = lane_index(packed)
        head, tail = jnp.zeros((packed, LANES), F32), jnp.zeros((packed, LANES), F32)
        for j in range(plan.groups):
            rows = slice(j * packed, (j + 1) * packed)
            first = lane // m == 2 * j
            second = lane // m == 2 * j + 1
            tail = jnp.where(first, pltpu.roll(brick[rows, width - LANES :], (2 * j * m + m) % LANES, 1), tail)
            head = jnp.where(second, pltpu.roll(brick[rows, :LANES], (2 * j + 1) * m % LANES, 1), head)
        self.pack[e, 0] = tail
        self.pack[e, 1] = head
        self.begin(self.y)
        self.begin(self.x)
        self.begin(self.z)

    def middle(self):
        plan, e = self.plan, self.number
        self.arrive(self.y)
        lane = lane_index(plan.packed)
        self.side[e, 1, 1] = jnp.where(lane // plan.margin % 2 == 0, self.left[e], self.right[e])
        self.begin(self.side_x)
        self.begin(self.side_z)
        for k in range(2):
            self.arrive(self.z[k : k + 1])
            self.begin(self.far_x[k])

    def last(self):
        for k in range(2):
            self.arrive(self.side_z[k : k + 1])
            self.begin(self.far_side[k])


def psf_first(plan, p_ref, wy_ref, tz_ref, y_ref, sre_ref, sim_ref):
    extent = plan.extent
    total = jnp.sum(jnp.sum(p_ref[...], axis=0, keepdims=True), axis=1, keepdims=True)
    tiles = extent // plan.groups
    values = jnp.concatenate([p_ref[:, t * LANES : (t + 1) * LANES] for t in range(tiles)], axis=0)
    lane = lane_index(values.shape[0])
    for j in range(plan.groups):
        high, low = split(jnp.where(lane // extent == j, values, 0.0))
        out = dot(jnp.concatenate([high, low], axis=1), wy_ref[: 2 * LANES, :]) + dot(high, wy_ref[2 * LANES :, :])
        out = out / total
        for t in range(tiles):
            a = plan.groups * t + j
            y_ref[a * extent : (a + 1) * extent, :] = out[t * extent : (t + 1) * extent]

    def along_z(a):
        re, im = apply_left(tz_ref[...], y_ref[pl.ds(aligned(a * extent, 8), extent), :], -1)
        sre_ref[pl.ds(a, plan.length_z, stride=plan.pitch_psf), :] = re
        sim_ref[pl.ds(a, plan.length_z, stride=plan.pitch_psf), :] = im

    loop(extent, along_z, 8)


def psf_second(plan, tx_ref, sre_ref, sim_ref, kre_ref, kim_ref):
    def along_x(l):
        rows = pl.ds(aligned(l * plan.pitch_psf, 8), plan.extent)
        values = jnp.concatenate([sre_ref[rows, :], sim_ref[rows, :]], axis=1)
        re, im = apply_left(tx_ref[...], values, -1)
        kre_ref[pl.ds(l, plan.length_x, stride=plan.pitch), :] = re
        kim_ref[pl.ds(l, plan.length_x, stride=plan.pitch), :] = im

    loop(plan.length_z, along_x, 8)


def block_y(plan, values, packed, wy_ref):
    core2, wide = 2 * plan.brick_y, plan.brick_y + LANES
    core_high, core_low = split(values)
    lane = lane_index(plan.packed)
    side = jnp.concatenate([jnp.where(lane // plan.extent == j, packed, 0.0) for j in range(plan.groups)], axis=0)
    side_high, side_low = split(side)
    return (
        dot(jnp.concatenate([core_high, core_low], axis=1), wy_ref[:core2, :])
        + dot(jnp.concatenate([core_high, side_high], axis=1), wy_ref[core2 : core2 + wide, :])
        + dot(jnp.concatenate([side_low, side_high], axis=1), wy_ref[core2 + wide :, :])
    )


def transform(plan, conj, valid_z, tables, spectrum, scratch):
    tx_ref, tz_ref, bz_ref, bx_ref, by_ref = tables
    kre_ref, kim_ref = spectrum
    y_ref, sre_ref, sim_ref, ire_ref, iim_ref, f_ref = scratch
    length_z, length_x, pitch, back = plan.length_z, plan.length_x, plan.pitch, plan.pitch_back
    bz, bx = plan.brick_z, plan.brick_x

    for zb in range(3):
        @pl.when(valid_z[zb])
        def _(zb=zb):
            def along_x(z):
                rows = pl.ds(aligned(z * bx, 8), bx)
                values = jnp.concatenate([y_ref[zb, xb, rows, :] for xb in range(3)], axis=0)
                re, im = apply_left(tx_ref[...], values, -1)
                sre_ref[pl.ds(zb * bz + z, length_x, stride=pitch), :] = re
                sim_ref[pl.ds(zb * bz + z, length_x, stride=pitch), :] = im

            loop(bz, along_x, UNROLL)

    group = math.gcd(length_x, UNROLL)

    def along_z(step):
        products = []
        for i in range(group):
            k = step * group + i
            rows = pl.ds(aligned(k * pitch, 8), length_z)
            values = jnp.concatenate([sre_ref[rows, :], sim_ref[rows, :]], axis=1)
            re, im = apply_left(tz_ref[...], values, -1)
            kre, kim = kre_ref[rows, :], kim_ref[rows, :]
            if conj:
                pre, pim = re * kre + im * kim, im * kre - re * kim
            else:
                pre, pim = re * kre - im * kim, re * kim + im * kre
            products.append(jnp.concatenate([pre, pim], axis=1))
        for i in range(group):
            re, im = apply_left(bz_ref[...], products[i], 1)
            ire_ref[pl.ds(step * group + i, bz, stride=back), :] = re
            iim_ref[pl.ds(step * group + i, bz, stride=back), :] = im

    loop(length_x // group, along_z, 1)

    def back_x(z):
        rows = pl.ds(aligned(z * back, 8), length_x)
        values = jnp.concatenate([ire_ref[rows, :], iim_ref[rows, :]], axis=1)
        re, im = apply_left(bx_ref[...], values, 1)
        f_ref[pl.ds(aligned(z * bx, 8), bx), :] = jnp.concatenate([re, im], axis=1)

    loop(bz, back_x, UNROLL)
    high, low = split(f_ref[...])
    by = plan.brick_y
    both = dot(high, by_ref[...])
    return both[:, :by] + both[:, by:] + dot(low, by_ref[:, :by])


def kernel(plan, *rest):
    sources = rest[:12]
    out_ref, across_ref, along_ref, top_ref = rest[12:16]
    held = rest[16:28]
    e_ref, m_ref, p_ref, psf_y, psf_x, psf_z, wy_ref = held[:7]
    tables = held[7:]
    (block, side, left, right, pack, ratio, py_ref, pre_ref, pim_ref, kre_ref, kim_ref,
     y_ref, sre_ref, sim_ref, ire_ref, iim_ref, f_ref,
     most_z, most_x, most_y, send, recv, most_send, most_recv, fetch) = rest[28:]
    fetched = [pltpu.make_async_copy(sources[i], held[i], fetch.at[i]) for i in range(12)]
    for i in (0, 2, 3, 5, 4, 6, 1, 7, 8, 9, 10, 11):
        fetched[i].start()
    most = {"gz": most_z, "gx": most_x, "gy": most_y}
    count = plan.mesh

    barrier = pltpu.get_barrier_semaphore()
    peers = 0
    for axis in AXES:
        for d in range(1, count[axis]):
            other = (lax.axis_index(axis) + d) % count[axis]
            pl.semaphore_signal(barrier, inc=1, device_id={axis: other}, device_id_type=pl.DeviceIdType.MESH)
            peers += 1
    pl.semaphore_wait(barrier, peers)

    ends = {axis: (lax.axis_index(axis) > 0, lax.axis_index(axis) < count[axis] - 1) for axis in AXES}
    valid_z = (ends["gz"][0], ends["gz"][0] | True, ends["gz"][1])
    valid_x = (ends["gx"][0], ends["gx"][0] | True, ends["gx"][1])
    refs = (block, side, left, right, pack, send, recv)
    first, second = Exchange(plan, 0, refs, ends), Exchange(plan, 1, refs, ends)

    fetched[0].wait()
    first.start(e_ref)
    for target, has in ((left, ends["gy"][0]), (right, ends["gy"][1])):
        @pl.when(jnp.logical_not(has))
        def _(target=target):
            target[...] = jnp.zeros_like(target)
    for zb in (0, 2):
        @pl.when(jnp.logical_not(valid_z[zb]))
        def _(zb=zb):
            def clear(k):
                rows = pl.ds(aligned(k * plan.pitch + zb * plan.brick_z, 8), plan.brick_z)
                zero = jnp.zeros((plan.brick_z, plan.lanes), F32)
                sre_ref[rows, :] = zero
                sim_ref[rows, :] = zero

            loop(plan.length_x, clear, 8)
    for xb in (0, 2):
        @pl.when(jnp.logical_not(valid_x[xb]))
        def _(xb=xb):
            for zb in range(3):
                y_ref[zb, xb] = jnp.zeros((plan.rows, 2 * plan.lanes), F32)

    def along_y(exchange, zb, xb, brick):
        @pl.when(jnp.logical_and(valid_z[zb], valid_x[xb]))
        def _():
            e = exchange.number
            values = brick[...] if (zb, xb) == (1, 1) else block[e, zb, xb]
            y_ref[zb, xb] = block_y(plan, values, side[e, zb, xb], wy_ref)

    def rest_of(exchange, brick):
        along_y(exchange, 1, 1, brick)
        along_y(exchange, 0, 1, brick)
        along_y(exchange, 2, 1, brick)
        exchange.arrive(exchange.x)
        exchange.arrive(exchange.side_x)
        along_y(exchange, 1, 0, brick)
        along_y(exchange, 1, 2, brick)
        for k, zb in enumerate((0, 2)):
            exchange.arrive(exchange.far_x[k])
            exchange.arrive(exchange.far_side[k])
            along_y(exchange, zb, 0, brick)
            along_y(exchange, zb, 2, brick)

    scratch = (y_ref, sre_ref, sim_ref, ire_ref, iim_ref, f_ref)
    for i in (2, 3, 5):
        fetched[i].wait()
    psf_first(plan, p_ref, psf_y, psf_z, py_ref, pre_ref, pim_ref)
    first.middle()
    fetched[4].wait()
    psf_second(plan, psf_x, pre_ref, pim_ref, kre_ref, kim_ref)
    first.last()
    for i in (6, 1, 7, 8, 9, 10, 11):
        fetched[i].wait()
    rest_of(first, e_ref)
    blurred = transform(plan, False, valid_z, tables, (kre_ref, kim_ref), scratch)
    ratio[...] = m_ref[...] / blurred

    second.start(ratio)
    second.middle()
    second.last()
    rest_of(second, ratio)
    correction = transform(plan, True, valid_z, tables, (kre_ref, kim_ref), scratch)
    updated = (e_ref[...] * correction).reshape(plan.brick_z, plan.brick_x, plan.brick_y)
    out_ref[...] = updated

    most_x[0] = jnp.max(updated, axis=1)
    most_y[0] = jnp.zeros((plan.brick_z, LANES), F32)
    most_y[0, :, : plan.brick_x] = jnp.max(updated, axis=2)
    most_z[0] = jnp.max(updated, axis=0)
    copies = {}
    slot = 0
    for axis in AXES:
        copies[axis] = []
        for d in range(1, count[axis]):
            item = pltpu.make_async_remote_copy(
                src_ref=most[axis].at[0],
                dst_ref=most[axis].at[d],
                send_sem=most_send.at[slot],
                recv_sem=most_recv.at[slot],
                device_id={axis: (lax.axis_index(axis) + d) % count[axis]},
                device_id_type=pl.DeviceIdType.MESH,
            )
            item.start()
            copies[axis].append(item)
            slot += 1
    first.leave()
    second.leave()
    found = {}
    for axis in AXES:
        value = most[axis][0]
        for d, item in enumerate(copies[axis]):
            item.wait_recv()
            value = jnp.maximum(value, most[axis][d + 1])
        found[axis] = value
    across_ref[...] = found["gx"]
    along_ref[...] = found["gy"][:, : plan.brick_x]
    piece = plan.brick_y // count["gz"]
    for i in range(count["gz"]):
        @pl.when(lax.axis_index("gz") == i)
        def _(i=i):
            top_ref[...] = found["gz"][:, i * piece : (i + 1) * piece]
    for axis in AXES:
        for item in copies[axis]:
            item.wait_send()


def deliver(count, *refs):
    sources, targets, sems = refs[:count], refs[count : 2 * count], refs[-1]
    outward = [pltpu.make_async_copy(sources[i], targets[i], sems.at[i]) for i in range(count)]
    for item in outward:
        item.start()
    for item in outward:
        item.wait()


def shards(sizes, estimate, measured, point_spread):
    plan = Plan(estimate.shape, point_spread.shape[0], sizes)
    bz, bx, by, rows = plan.brick_z, plan.brick_x, plan.brick_y, plan.rows
    args = (estimate.reshape(rows, by), measured.reshape(rows, by), point_spread, *plan.tables())
    vmem = pl.BlockSpec(memory_space=pltpu.VMEM)
    outs = [(bz, bx, by), (bz, by), (bz, bx), (bx, by // sizes["gz"])]
    spread = (plan.length_x * plan.pitch, plan.lanes)
    psf_spread = (plan.length_z * plan.pitch_psf, plan.lanes)
    back = (bz * plan.pitch_back, plan.lanes)
    shapes = [
        (2, 3, 3, rows, by), (2, 3, 3, plan.packed, LANES), (2, plan.packed, LANES), (2, plan.packed, LANES),
        (2, 2, plan.packed, LANES), (rows, by), (plan.extent * plan.extent, 2 * plan.lanes), psf_spread, psf_spread,
        spread, spread, (3, 3, rows, 2 * plan.lanes), spread, spread, back, back, (rows, 2 * plan.lanes),
        (sizes["gz"], bx, by), (sizes["gx"], bz, by), (sizes["gy"], bz, LANES),
    ]
    peers = sum(sizes[axis] - 1 for axis in AXES)
    sems = pltpu.SemaphoreType.DMA
    held = [pltpu.VMEM(item.shape, item.dtype) for item in args]
    results = pl.pallas_call(
        functools.partial(kernel, plan),
        out_shape=[pltpu.VMEM(shape, F32) for shape in outs],
        in_specs=[pl.BlockSpec(memory_space=pltpu.HBM)] * len(args),
        out_specs=[vmem] * len(outs),
        scratch_shapes=held + [pltpu.VMEM(shape, F32) for shape in shapes]
        + [sems((2, 18)), sems((2, 18)), sems((peers,)), sems((peers,)), sems((len(args),))],
        compiler_params=pltpu.CompilerParams(collective_id=0, has_side_effects=True, vmem_limit_bytes=GRANT),
    )(*args)
    return pl.pallas_call(
        functools.partial(deliver, len(outs)),
        out_shape=[jax.ShapeDtypeStruct(shape, F32) for shape in outs],
        in_specs=[vmem] * len(outs),
        out_specs=[pl.BlockSpec(memory_space=pltpu.HBM)] * len(outs),
        scratch_shapes=[sems((len(outs),))],
        compiler_params=pltpu.CompilerParams(vmem_limit_bytes=ROOM),
    )(*results)


def solution(mesh):
    in_specs = (P("gz", "gx", "gy"), P("gz", "gx", "gy"), P())
    out_specs = (P("gz", "gx", "gy"), P("gz", "gy"), P("gz", "gx"), P("gx", ("gy", "gz")))
    body = functools.partial(shards, {axis: mesh.shape[axis] for axis in AXES})
    return jax.shard_map(lambda *args: tuple(body(*args)), mesh=mesh, in_specs=in_specs, out_specs=out_specs, check_vma=False)
```

```python
import functools
import math

import jax
import jax.numpy as jnp
import ml_dtypes
import numpy as np
from jax import lax
from jax.experimental import pallas as pl
from jax.experimental.pallas import tpu as pltpu
from jax.sharding import PartitionSpec as P

LANES = 128
UNROLL = 16
NEAR = 4
PARTS = 3
CHUNKS = 2
SLOTS = 18 + 6 * CHUNKS
GRANT = 66879488
ROOM = 1 << 20
BF16 = jnp.bfloat16
F32 = jnp.float32


def round_up(value, step):
    return -(-value // step) * step


def angles(frequencies, positions, length):
    grid = np.mod(np.outer(frequencies, positions), length)
    return grid * (2.0 * math.pi / length)


def parts_of(table):
    high = table.astype(np.float32).astype(ml_dtypes.bfloat16)
    low = (table - high.astype(np.float64)).astype(np.float32).astype(ml_dtypes.bfloat16)
    return high, low


def left_table(frequencies, positions, length, transpose=False):
    theta = angles(frequencies, positions, length)
    if transpose:
        theta = theta.T
    high, low = parts_of(np.concatenate([np.cos(theta), np.sin(theta)], axis=0))
    return np.concatenate([high, high, low], axis=1)


def forward_rows(positions, length, bins, lanes, rows):
    theta = angles(positions, np.arange(bins), length)
    table = np.zeros((rows, 2 * lanes))
    table[: len(positions), :bins] = np.cos(theta)
    table[: len(positions), lanes : lanes + bins] = -np.sin(theta)
    return parts_of(table)


def inverse_rows(positions, length, bins, lanes, scale):
    theta = angles(np.arange(bins), positions, length)
    weight = np.full((bins, 1), 2.0)
    weight[0] = 1.0
    if length % 2 == 0:
        weight[-1] = 1.0
    table = np.zeros((2 * lanes, len(positions)))
    table[:bins] = weight * np.cos(theta) * scale
    table[lanes : lanes + bins] = -weight * np.sin(theta) * scale
    return parts_of(table)


class Plan:
    def __init__(self, brick, extent, mesh):
        self.mesh = mesh
        self.extent = extent
        self.margin = extent // 2
        self.brick_z, self.brick_x, self.brick_y = brick
        self.rows = self.brick_z * self.brick_x
        self.length_z = self.brick_z + extent
        self.length_x = self.brick_x + extent
        self.length_y = self.brick_y + extent
        self.bins = self.length_y // 2 + 1
        self.lanes = round_up(self.bins, LANES)
        self.pitch = self.length_z + 8
        self.pitch_back = self.length_x + 8
        self.pitch_psf = extent + 8
        self.groups = LANES // extent
        self.packed = self.rows // self.groups
        self.dense = self.packed // 2

    def tables(self):
        m = self.margin
        offsets = np.arange(self.extent) - m
        high, low = forward_rows(offsets, self.length_y, self.bins, self.lanes, self.extent)
        high, low = np.tile(high, (self.groups, 1)), np.tile(low, (self.groups, 1))
        frequency_x = np.arange(self.length_x)
        frequency_z = np.arange(self.length_z)
        psf_y = np.concatenate([high, high, low], axis=0)
        psf_x = left_table(frequency_x, offsets, self.length_x)
        psf_z = left_table(frequency_z, offsets, self.length_z)
        core = np.arange(self.brick_y) + m
        side = np.concatenate([np.arange(m), np.arange(m) + m + self.brick_y])
        core_high, core_low = forward_rows(core, self.length_y, self.bins, self.lanes, self.brick_y)
        side_high, side_low = forward_rows(side, self.length_y, self.bins, self.lanes, self.extent)
        side_high, side_low = np.tile(side_high, (self.groups, 1)), np.tile(side_low, (self.groups, 1))
        wide = np.concatenate([core_high, core_high, core_low, side_high, side_high, side_low], axis=0)
        along_x = left_table(frequency_x, frequency_x, self.length_x)
        along_z = left_table(frequency_z, frequency_z, self.length_z)
        back_z = left_table(frequency_z, np.arange(self.brick_z) + m, self.length_z, True)
        back_x = left_table(frequency_x, np.arange(self.brick_x) + m, self.length_x, True)
        scale = 1.0 / float(self.length_z * self.length_x * self.length_y)
        high, low = inverse_rows(core, self.length_y, self.bins, self.lanes, scale)
        back_y = np.concatenate([high, low], axis=1)
        return psf_y, psf_x, psf_z, wide, along_x, along_z, back_z, back_x, back_y


def split(values):
    high = values.astype(BF16)
    low = (values - high.astype(F32)).astype(BF16)
    return high, low


def dot(left, right):
    return jnp.dot(left, right, preferred_element_type=F32)


def apply_left(table, values, sign):
    lanes = values.shape[1] // 2
    high, low = split(values)
    out = dot(table, jnp.concatenate([high, low, high], axis=0))
    half = out.shape[0] // 2
    top_re, top_im = out[:half, :lanes], out[:half, lanes:]
    low_re, low_im = out[half:, :lanes], out[half:, lanes:]
    if sign < 0:
        return top_re + low_im, top_im - low_re
    return top_re - low_im, top_im + low_re


def loop(count, body, unroll):
    def step(i, carry):
        body(i)
        return carry

    lax.fori_loop(0, count, step, 0, unroll=math.gcd(count, unroll))


def aligned(value, step):
    return pl.multiple_of(value, step)


AXES = ("gz", "gx", "gy")


def lane_index(rows):
    return lax.broadcasted_iota(jnp.int32, (rows, LANES), 1)


def parity(k):
    return lax.axis_index("gx") % 2 == k


class Exchange:
    def __init__(self, plan, number, refs, ends):
        self.plan, self.number, self.ends = plan, number, ends
        self.block, self.side, self.left, self.right, self.pack, self.send, self.recv = refs

    def copy(self, source, target, slot, place):
        return pltpu.make_async_remote_copy(
            src_ref=source,
            dst_ref=target,
            send_sem=self.send.at[self.number, slot],
            recv_sem=self.recv.at[self.number, slot],
            device_id=place,
            device_id_type=pl.DeviceIdType.MESH,
        )

    def pair(self, axis, source, targets, slot, guard=None, near=False):
        low, high = self.ends[axis]
        out = []
        for k, step in ((0, 1), (1, -1)):
            sends, receives = (high, low) if step == 1 else (low, high)
            if guard is not None:
                sends, receives = jnp.logical_and(sends, guard), jnp.logical_and(receives, guard)
            if near:
                sends, receives = jnp.logical_and(sends, parity(k)), jnp.logical_and(receives, parity(1 - k))
            out.append((sends, receives, self.copy(source, targets[k], slot + k, {axis: lax.axis_index(axis) + step})))
        return out

    def strips(self, spot, turn, slot):
        e, out = self.number, []
        low, high = self.ends["gy"]
        for k, step, target in ((0, 1, self.left), (1, -1, self.right)):
            sends, receives = (high, low) if step == 1 else (low, high)
            place = {"gy": lax.axis_index("gy") + step}
            if turn is not None:
                axis, shift = turn
                below, above = self.ends[axis]
                leaves, comes = (above, below) if shift == 1 else (below, above)
                if axis == "gx":
                    leaves = jnp.logical_and(leaves, parity(1 if shift == 1 else 0))
                    comes = jnp.logical_and(comes, parity(0 if shift == 1 else 1))
                sends, receives = jnp.logical_and(sends, leaves), jnp.logical_and(receives, comes)
                place[axis] = lax.axis_index(axis) + shift
            out.append((sends, receives, self.copy(self.pack.at[e, k], target.at[e, spot], slot + k, place)))
        return out

    def plans(self, brick):
        e, block, side = self.number, self.block, self.side
        low, high = self.ends["gz"]
        span = self.plan.rows // CHUNKS
        cuts = [pl.ds(c * span, span) for c in range(CHUNKS)]
        slots = iter(range(0, SLOTS, 2))
        self.y = self.strips(1, None, next(slots))
        self.x = self.pair("gx", brick, (block.at[e, 1, 0], block.at[e, 1, 2]), next(slots))
        self.side_z = [self.strips(0, ("gz", 1), next(slots)), self.strips(2, ("gz", -1), next(slots))]
        self.cross = [self.strips(3, ("gx", 1), next(slots)), self.strips(4, ("gx", -1), next(slots))]
        self.side_x = self.pair("gx", side.at[e, 1, 1], (side.at[e, 1, 0], side.at[e, 1, 2]), next(slots), None, True)
        self.z = [
            self.pair("gz", brick.at[cut], (block.at[e, 0, 1, cut], block.at[e, 2, 1, cut]), next(slots)) for cut in cuts
        ]
        self.far_x, self.far_side = [], []
        for zb, guard in ((0, low), (2, high)):
            self.far_x.append([
                self.pair("gx", block.at[e, zb, 1, cut], (block.at[e, zb, 0, cut], block.at[e, zb, 2, cut]), next(slots), guard)
                for cut in cuts
            ])
            self.far_side.append(
                self.pair("gx", side.at[e, zb, 1], (side.at[e, zb, 0], side.at[e, zb, 2]), next(slots), guard)
            )

    def begin(self, copies):
        for sends, _, item in copies:
            @pl.when(sends)
            def _(item=item):
                item.start()

    def arrive(self, copies):
        for _, receives, item in copies:
            @pl.when(receives)
            def _(item=item):
                item.wait_recv()

    def leave(self):
        far = [copies for both in self.far_x for copies in both]
        for copies in (self.y, self.x, *self.side_z, *self.cross, self.side_x, *self.z, *far, *self.far_side):
            for sends, _, item in copies:
                @pl.when(sends)
                def _(item=item):
                    item.wait_send()

    def start(self, brick):
        plan, e = self.plan, self.number
        self.plans(brick)
        m, dense, width = plan.margin, plan.dense, plan.brick_y
        lane = lane_index(dense)
        head, tail = jnp.zeros((dense, LANES), F32), jnp.zeros((dense, LANES), F32)
        for j in range(LANES // m):
            rows = slice(j * dense, (j + 1) * dense)
            here = lane // m == j
            tail = jnp.where(here, pltpu.roll(brick[rows, width - LANES :], (j * m + m) % LANES, 1), tail)
            head = jnp.where(here, pltpu.roll(brick[rows, :LANES], j * m, 1) if j else brick[rows, :LANES], head)
        self.pack[e, 0] = tail
        self.pack[e, 1] = head
        self.begin(self.y)
        for copies in (*self.side_z, *self.cross):
            self.begin(copies)
        for copies in self.z:
            self.begin(copies)
        self.begin(self.x)

    def join(self, spot, zb, xb):
        m, e = self.plan.margin, self.number
        left, right = self.left[e, spot], self.right[e, spot]
        even = lane_index(self.plan.dense) // m % 2 == 0
        upper = jnp.where(even, left, pltpu.roll(right, m, 1))
        lower = jnp.where(even, pltpu.roll(left, LANES - m, 1), right)
        self.side[e, zb, xb] = jnp.concatenate([upper, lower], axis=0)

    def middle(self):
        self.arrive(self.y)
        self.join(1, 1, 1)
        self.begin(self.side_x)

    def forward(self, c):
        for k in range(2):
            self.arrive(self.z[c][k : k + 1])
            self.begin(self.far_x[k][c])

    def last(self):
        for k in range(2):
            @pl.when(self.ends["gz"][k])
            def _(k=k):
                self.arrive(self.side_z[k])
                self.join(2 * k, 2 * k, 1)
            self.begin(self.far_side[k])

    def row(self):
        self.arrive(self.x)
        self.arrive(self.side_x)
        for k in range(2):
            @pl.when(jnp.logical_and(self.ends["gx"][k], parity(k)))
            def _(k=k):
                self.arrive(self.cross[k])
                self.join(3 + k, 1, 2 * k)

    def far(self, k):
        for copies in self.far_x[k]:
            self.arrive(copies)
        self.arrive(self.far_side[k])


def psf_first(plan, p_ref, wy_ref, tz_ref, y_ref, sre_ref, sim_ref):
    extent = plan.extent
    total = jnp.sum(jnp.sum(p_ref[...], axis=0, keepdims=True), axis=1, keepdims=True)
    tiles = extent // plan.groups
    values = jnp.concatenate([p_ref[:, t * LANES : (t + 1) * LANES] for t in range(tiles)], axis=0)
    lane = lane_index(values.shape[0])
    for j in range(plan.groups):
        high, low = split(jnp.where(lane // extent == j, values, 0.0))
        out = dot(jnp.concatenate([high, low], axis=1), wy_ref[: 2 * LANES, :]) + dot(high, wy_ref[2 * LANES :, :])
        out = out / total
        for t in range(tiles):
            a = plan.groups * t + j
            y_ref[a * extent : (a + 1) * extent, :] = out[t * extent : (t + 1) * extent]

    def along_z(a):
        re, im = apply_left(tz_ref[...], y_ref[pl.ds(aligned(a * extent, 8), extent), :], -1)
        sre_ref[pl.ds(a, plan.length_z, stride=plan.pitch_psf), :] = re
        sim_ref[pl.ds(a, plan.length_z, stride=plan.pitch_psf), :] = im

    loop(extent, along_z, UNROLL)


def psf_second(plan, part, tx_ref, sre_ref, sim_ref, kre_ref, kim_ref):
    first = part * plan.length_z // PARTS
    count = (part + 1) * plan.length_z // PARTS - first

    def along_x(i):
        l = first + i
        rows = pl.ds(aligned(l * plan.pitch_psf, 8), plan.extent)
        values = jnp.concatenate([sre_ref[rows, :], sim_ref[rows, :]], axis=1)
        re, im = apply_left(tx_ref[...], values, -1)
        kre_ref[pl.ds(l, plan.length_x, stride=plan.pitch), :] = re
        kim_ref[pl.ds(l, plan.length_x, stride=plan.pitch), :] = im

    loop(count, along_x, UNROLL)


def block_y(plan, values, packed, wy_ref):
    core2, wide = 2 * plan.brick_y, plan.brick_y + LANES
    core_high, core_low = split(values)
    lane = lane_index(plan.packed)
    side = jnp.concatenate([jnp.where(lane // plan.extent == j, packed, 0.0) for j in range(plan.groups)], axis=0)
    side_high, side_low = split(side)
    return (
        dot(jnp.concatenate([core_high, core_low], axis=1), wy_ref[:core2, :])
        + dot(jnp.concatenate([core_high, side_high], axis=1), wy_ref[core2 : core2 + wide, :])
        + dot(jnp.concatenate([side_low, side_high], axis=1), wy_ref[core2 + wide :, :])
    )


def along_rows(plan, zb, tx_ref, scratch):
    y_ref, sre_ref, sim_ref = scratch[:3]
    bz, bx = plan.brick_z, plan.brick_x

    def along_x(z):
        rows = pl.ds(aligned(z * bx, 8), bx)
        values = jnp.concatenate([y_ref[zb, xb, rows, :] for xb in range(3)], axis=0)
        re, im = apply_left(tx_ref[...], values, -1)
        sre_ref[pl.ds(zb * bz + z, plan.length_x, stride=plan.pitch), :] = re
        sim_ref[pl.ds(zb * bz + z, plan.length_x, stride=plan.pitch), :] = im

    loop(bz, along_x, UNROLL)


def transform(plan, conj, tables, spectrum, scratch):
    tz_ref, bz_ref, bx_ref, by_ref = tables
    kre_ref, kim_ref = spectrum
    sre_ref, sim_ref, ire_ref, iim_ref, f_ref, q_ref = scratch[1:]
    length_z, length_x, pitch, back = plan.length_z, plan.length_x, plan.pitch, plan.pitch_back
    bz, bx, lanes = plan.brick_z, plan.brick_x, plan.lanes
    group = math.gcd(length_x, UNROLL)

    def along_z(step, i):
        k = step * group + i
        rows = pl.ds(aligned(k * pitch, 8), length_z)
        values = jnp.concatenate([sre_ref[rows, :], sim_ref[rows, :]], axis=1)
        re, im = apply_left(tz_ref[...], values, -1)
        kre, kim = kre_ref[rows, :], kim_ref[rows, :]
        if conj:
            pre, pim = re * kre + im * kim, im * kre - re * kim
        else:
            pre, pim = re * kre - im * kim, re * kim + im * kre
        high, low = split(jnp.concatenate([pre, pim], axis=1))
        q_ref[step % 2, i, :length_z] = high
        q_ref[step % 2, i, length_z:] = low

    def back_z(step, i):
        pair = q_ref[step % 2, i]
        out = dot(bz_ref[...], jnp.concatenate([pair, pair[:length_z]], axis=0))
        k = step * group + i
        ire_ref[pl.ds(k, bz, stride=back), :] = out[:bz, :lanes] - out[bz:, lanes:]
        iim_ref[pl.ds(k, bz, stride=back), :] = out[:bz, lanes:] + out[bz:, :lanes]

    steps = length_x // group
    for i in range(group):
        along_z(0, i)

    for step in range(steps - 1):
        for i in range(group):
            along_z(step + 1, i)
            back_z(step, i)

    for i in range(group):
        back_z(steps - 1, i)

    def back_x(z):
        rows = pl.ds(aligned(z * back, 8), length_x)
        values = jnp.concatenate([ire_ref[rows, :], iim_ref[rows, :]], axis=1)
        re, im = apply_left(bx_ref[...], values, 1)
        f_ref[pl.ds(aligned(z * bx, 8), bx), :] = jnp.concatenate([re, im], axis=1)

    loop(bz, back_x, UNROLL)
    high, low = split(f_ref[...])
    by = plan.brick_y
    both = dot(high, by_ref[...])
    return both[:, :by] + both[:, by:] + dot(low, by_ref[:, :by])


def kernel(plan, *rest):
    sources = rest[:12]
    out_ref, across_ref, along_ref, top_ref = rest[12:16]
    held = rest[16:28]
    e_ref, m_ref, p_ref, psf_y, psf_x, psf_z, wy_ref = held[:7]
    tables = held[7:]
    (block, side, left, right, pack, ratio, py_ref, pre_ref, pim_ref, kre_ref, kim_ref,
     y_ref, sre_ref, sim_ref, ire_ref, iim_ref, f_ref, q_ref,
     most_z, most_x, most_y, send, recv, most_send, most_recv, fetch) = rest[28:]
    fetched = [pltpu.make_async_copy(sources[i], held[i], fetch.at[i]) for i in range(12)]
    for i in (0, 2, 3, 5, 4, 6, 1, 7, 8, 9, 10, 11):
        fetched[i].start()
    most = {"gz": most_z, "gx": most_x, "gy": most_y}
    count = plan.mesh

    ends = {axis: (lax.axis_index(axis) > 0, lax.axis_index(axis) < count[axis] - 1) for axis in AXES}
    barrier = pltpu.get_barrier_semaphore()
    greet = []
    for axis in AXES:
        if max(count[axis] for axis in AXES) <= NEAR:
            for k, d in enumerate((-1, 1)):
                greet.append((ends[axis][k], {axis: lax.axis_index(axis) + d}))
        else:
            for d in range(1, count[axis]):
                greet.append((None, {axis: (lax.axis_index(axis) + d) % count[axis]}))
    for axis in ("gz", "gx"):
        for k, d in enumerate((-1, 1)):
            for n, step in enumerate((-1, 1)):
                place = {axis: lax.axis_index(axis) + d, "gy": lax.axis_index("gy") + step}
                greet.append((jnp.logical_and(ends[axis][k], ends["gy"][n]), place))
    total = 0
    for has, place in greet:
        def signal(place=place):
            pl.semaphore_signal(barrier, inc=1, device_id=place, device_id_type=pl.DeviceIdType.MESH)

        if has is None:
            signal()
            total = total + 1
        else:
            pl.when(has)(signal)
            total = total + has.astype(jnp.int32)
    pl.semaphore_wait(barrier, total)

    valid_z = (ends["gz"][0], ends["gz"][0] | True, ends["gz"][1])
    valid_x = (ends["gx"][0], ends["gx"][0] | True, ends["gx"][1])
    refs = (block, side, left, right, pack, send, recv)
    first, second = Exchange(plan, 0, refs, ends), Exchange(plan, 1, refs, ends)

    fetched[0].wait()
    first.start(e_ref)
    for target, has in ((left, ends["gy"][0]), (right, ends["gy"][1])):
        @pl.when(jnp.logical_not(has))
        def _(target=target):
            target[...] = jnp.zeros_like(target)
    for zb in (0, 2):
        @pl.when(jnp.logical_not(valid_z[zb]))
        def _(zb=zb):
            def clear(k):
                rows = pl.ds(aligned(k * plan.pitch + zb * plan.brick_z, 8), plan.brick_z)
                zero = jnp.zeros((plan.brick_z, plan.lanes), F32)
                sre_ref[rows, :] = zero
                sim_ref[rows, :] = zero

            loop(plan.length_x, clear, 8)
    for xb in (0, 2):
        @pl.when(jnp.logical_not(valid_x[xb]))
        def _(xb=xb):
            for e in range(2):
                for zb in range(3):
                    block[e, zb, xb] = jnp.zeros((plan.rows, plan.brick_y), F32)
                    side[e, zb, xb] = jnp.zeros((plan.packed, LANES), F32)

    def along_y(exchange, zb, spots, brick):
        @pl.when(valid_z[zb])
        def _():
            e = exchange.number
            for xb in spots:
                values = brick[...] if (zb, xb) == (1, 1) else block[e, zb, xb]
                y_ref[zb, xb] = block_y(plan, values, side[e, zb, xb], wy_ref)

    scratch = (y_ref, sre_ref, sim_ref, ire_ref, iim_ref, f_ref, q_ref)
    tx_ref = tables[0]

    def rows_of(zb):
        @pl.when(valid_z[zb])
        def _():
            along_rows(plan, zb, tx_ref, scratch)

    def rest_of(exchange, brick):
        along_y(exchange, 1, (1,), brick)
        exchange.row()
        along_y(exchange, 1, (0, 2), brick)
        rows_of(1)
        along_y(exchange, 0, (1,), brick)
        along_y(exchange, 2, (1,), brick)
        for k, zb in enumerate((0, 2)):
            exchange.far(k)
            along_y(exchange, zb, (0, 2), brick)
            rows_of(zb)

    for i in (2, 3, 5):
        fetched[i].wait()
    psf_first(plan, p_ref, psf_y, psf_z, py_ref, pre_ref, pim_ref)
    fetched[4].wait()
    psf_second(plan, 0, psf_x, pre_ref, pim_ref, kre_ref, kim_ref)
    psf_second(plan, 1, psf_x, pre_ref, pim_ref, kre_ref, kim_ref)
    first.middle()
    for c in range(0, 1):
        first.forward(c)
    first.last()
    for c in range(1, 2):
        first.forward(c)
    psf_second(plan, 2, psf_x, pre_ref, pim_ref, kre_ref, kim_ref)
    for i in (6, 1, 7, 8, 9, 10, 11):
        fetched[i].wait()
    rest_of(first, e_ref)
    blurred = transform(plan, False, tables[1:], (kre_ref, kim_ref), scratch)
    ratio[...] = m_ref[...] / blurred

    second.start(ratio)
    second.middle()
    second.forward(0)
    second.last()
    second.forward(1)
    rest_of(second, ratio)
    correction = transform(plan, True, tables[1:], (kre_ref, kim_ref), scratch)
    updated = (e_ref[...] * correction).reshape(plan.brick_z, plan.brick_x, plan.brick_y)

    copies = {}
    slot = 0

    def share(axis):
        nonlocal slot
        copies[axis] = []
        for d in range(count[axis] - 1, 0, -1):
            item = pltpu.make_async_remote_copy(
                src_ref=most[axis].at[0],
                dst_ref=most[axis].at[d],
                send_sem=most_send.at[slot],
                recv_sem=most_recv.at[slot],
                device_id={axis: (lax.axis_index(axis) + d) % count[axis]},
                device_id_type=pl.DeviceIdType.MESH,
            )
            item.start()
            copies[axis].append((d, item))
            slot += 1

    most_y[0] = jnp.zeros((plan.brick_z, LANES), F32)
    most_y[0, :, : plan.brick_x] = jnp.max(updated, axis=2)
    share("gy")
    most_x[0] = jnp.max(updated, axis=1)
    share("gx")
    most_z[0] = jnp.max(updated, axis=0)
    share("gz")
    out_ref[...] = updated
    first.leave()
    second.leave()
    found = {}
    for axis in AXES:
        value = most[axis][0]
        for d, item in copies[axis]:
            item.wait_recv()
            value = jnp.maximum(value, most[axis][d])
        found[axis] = value
    across_ref[...] = found["gx"]
    along_ref[...] = found["gy"][:, : plan.brick_x]
    piece = plan.brick_y // count["gz"]
    for i in range(count["gz"]):
        @pl.when(lax.axis_index("gz") == i)
        def _(i=i):
            top_ref[...] = found["gz"][:, i * piece : (i + 1) * piece]
    for axis in AXES:
        for _, item in copies[axis]:
            item.wait_send()


def deliver(count, *refs):
    sources, targets, sems = refs[:count], refs[count : 2 * count], refs[-1]
    outward = [pltpu.make_async_copy(sources[i], targets[i], sems.at[i]) for i in range(count)]
    for item in outward:
        item.start()
    for item in outward:
        item.wait()


def shards(sizes, estimate, measured, point_spread):
    plan = Plan(estimate.shape, point_spread.shape[0], sizes)
    bz, bx, by, rows = plan.brick_z, plan.brick_x, plan.brick_y, plan.rows
    args = (estimate.reshape(rows, by), measured.reshape(rows, by), point_spread, *plan.tables())
    vmem = pl.BlockSpec(memory_space=pltpu.VMEM)
    outs = [(bz, bx, by), (bz, by), (bz, bx), (bx, by // sizes["gz"])]
    spread = (plan.length_x * plan.pitch, plan.lanes)
    psf_spread = (plan.length_z * plan.pitch_psf, plan.lanes)
    back = (bz * plan.pitch_back, plan.lanes)
    shapes = [
        (2, 3, 3, rows, by), (2, 3, 3, plan.packed, LANES), (2, 5, plan.dense, LANES), (2, 5, plan.dense, LANES),
        (2, 2, plan.dense, LANES), (rows, by), (plan.extent * plan.extent, 2 * plan.lanes), psf_spread, psf_spread,
        spread, spread, (3, 3, rows, 2 * plan.lanes), spread, spread, back, back, (rows, 2 * plan.lanes),
        (sizes["gz"], bx, by), (sizes["gx"], bz, by), (sizes["gy"], bz, LANES),
    ]
    peers = sum(sizes[axis] - 1 for axis in AXES)
    sems = pltpu.SemaphoreType.DMA
    held = [pltpu.VMEM(item.shape, item.dtype) for item in args]
    queue = (2, math.gcd(plan.length_x, UNROLL), 2 * plan.length_z, 2 * plan.lanes)
    scratch = [pltpu.VMEM(shape, F32) for shape in shapes]
    scratch.insert(17, pltpu.VMEM(queue, BF16))
    results = pl.pallas_call(
        functools.partial(kernel, plan),
        out_shape=[pltpu.VMEM(shape, F32) for shape in outs],
        in_specs=[pl.BlockSpec(memory_space=pltpu.HBM)] * len(args),
        out_specs=[vmem] * len(outs),
        scratch_shapes=held + scratch
        + [sems((2, SLOTS)), sems((2, SLOTS)), sems((peers,)), sems((peers,)), sems((len(args),))],
        compiler_params=pltpu.CompilerParams(collective_id=0, has_side_effects=True, vmem_limit_bytes=GRANT),
    )(*args)
    return pl.pallas_call(
        functools.partial(deliver, len(outs)),
        out_shape=[jax.ShapeDtypeStruct(shape, F32) for shape in outs],
        in_specs=[vmem] * len(outs),
        out_specs=[pl.BlockSpec(memory_space=pltpu.HBM)] * len(outs),
        scratch_shapes=[sems((len(outs),))],
        compiler_params=pltpu.CompilerParams(vmem_limit_bytes=ROOM),
    )(*results)


def solution(mesh):
    in_specs = (P("gz", "gx", "gy"), P("gz", "gx", "gy"), P())
    out_specs = (P("gz", "gx", "gy"), P("gz", "gy"), P("gz", "gx"), P("gx", ("gy", "gz")))
    body = functools.partial(shards, {axis: mesh.shape[axis] for axis in AXES})
    return jax.shard_map(lambda *args: tuple(body(*args)), mesh=mesh, in_specs=in_specs, out_specs=out_specs, check_vma=False)
```

```python
import functools
import math

import jax
import jax.numpy as jnp
import ml_dtypes
import numpy as np
from jax import lax
from jax.experimental import pallas as pl
from jax.experimental.pallas import tpu as pltpu
from jax.sharding import PartitionSpec as P

LANES = 128
UNROLL = 16
NEAR = 4
PARTS = 3
CHUNKS = 2
SLOTS = 18 + 6 * CHUNKS
GRANT = 66879488
ROOM = 1 << 20
BF16 = jnp.bfloat16
F32 = jnp.float32


def round_up(value, step):
    return -(-value // step) * step


def angles(frequencies, positions, length):
    grid = np.mod(np.outer(frequencies, positions), length)
    return grid * (2.0 * math.pi / length)


def parts_of(table):
    high = table.astype(np.float32).astype(ml_dtypes.bfloat16)
    low = (table - high.astype(np.float64)).astype(np.float32).astype(ml_dtypes.bfloat16)
    return high, low


def left_table(frequencies, positions, length, transpose=False):
    theta = angles(frequencies, positions, length)
    if transpose:
        theta = theta.T
    high, low = parts_of(np.concatenate([np.cos(theta), np.sin(theta)], axis=0))
    return np.concatenate([high, high, low], axis=1)


def forward_rows(positions, length, bins, lanes, rows):
    theta = angles(positions, np.arange(bins), length)
    table = np.zeros((rows, 2 * lanes))
    table[: len(positions), :bins] = np.cos(theta)
    table[: len(positions), lanes : lanes + bins] = -np.sin(theta)
    return parts_of(table)


def inverse_rows(positions, length, bins, lanes, scale):
    theta = angles(np.arange(bins), positions, length)
    weight = np.full((bins, 1), 2.0)
    weight[0] = 1.0
    if length % 2 == 0:
        weight[-1] = 1.0
    table = np.zeros((2 * lanes, len(positions)))
    table[:bins] = weight * np.cos(theta) * scale
    table[lanes : lanes + bins] = -weight * np.sin(theta) * scale
    return parts_of(table)


class Plan:
    def __init__(self, brick, extent, mesh):
        self.mesh = mesh
        self.extent = extent
        self.margin = extent // 2
        self.brick_z, self.brick_x, self.brick_y = brick
        self.rows = self.brick_z * self.brick_x
        self.length_z = self.brick_z + extent
        self.length_x = self.brick_x + extent
        self.length_y = self.brick_y + extent
        self.bins = self.length_y // 2 + 1
        self.lanes = round_up(self.bins, LANES)
        self.pitch = self.length_z + 8
        self.pitch_back = self.length_x + 8
        self.pitch_psf = extent + 8
        self.groups = LANES // extent
        self.packed = self.rows // self.groups
        self.dense = self.packed // 2

    def tables(self):
        m = self.margin
        offsets = np.arange(self.extent) - m
        high, low = forward_rows(offsets, self.length_y, self.bins, self.lanes, self.extent)
        high, low = np.tile(high, (self.groups, 1)), np.tile(low, (self.groups, 1))
        frequency_x = np.arange(self.length_x)
        frequency_z = np.arange(self.length_z)
        psf_y = np.concatenate([high, high, low], axis=0)
        psf_x = left_table(frequency_x, offsets, self.length_x)
        psf_z = left_table(frequency_z, offsets, self.length_z)
        core = np.arange(self.brick_y) + m
        side = np.concatenate([np.arange(m), np.arange(m) + m + self.brick_y])
        core_high, core_low = forward_rows(core, self.length_y, self.bins, self.lanes, self.brick_y)
        side_high, side_low = forward_rows(side, self.length_y, self.bins, self.lanes, self.extent)
        side_high, side_low = np.tile(side_high, (self.groups, 1)), np.tile(side_low, (self.groups, 1))
        wide = np.concatenate([core_high, core_high, core_low, side_high, side_high, side_low], axis=0)
        along_x = left_table(frequency_x, frequency_x, self.length_x)
        along_z = left_table(frequency_z, frequency_z, self.length_z)
        back_z = left_table(frequency_z, np.arange(self.brick_z) + m, self.length_z, True)
        back_x = left_table(frequency_x, np.arange(self.brick_x) + m, self.length_x, True)
        scale = 1.0 / float(self.length_z * self.length_x * self.length_y)
        high, low = inverse_rows(core, self.length_y, self.bins, self.lanes, scale)
        back_y = np.concatenate([high, low], axis=1)
        return psf_y, psf_x, psf_z, wide, along_x, along_z, back_z, back_x, back_y


def split(values):
    high = values.astype(BF16)
    low = (values - high.astype(F32)).astype(BF16)
    return high, low


def dot(left, right):
    return jnp.dot(left, right, preferred_element_type=F32)


def apply_left(table, values, sign):
    lanes = values.shape[1] // 2
    high, low = split(values)
    out = dot(table, jnp.concatenate([high, low, high], axis=0))
    half = out.shape[0] // 2
    top_re, top_im = out[:half, :lanes], out[:half, lanes:]
    low_re, low_im = out[half:, :lanes], out[half:, lanes:]
    if sign < 0:
        return top_re + low_im, top_im - low_re
    return top_re - low_im, top_im + low_re


def loop(count, body, unroll):
    def step(i, carry):
        body(i)
        return carry

    lax.fori_loop(0, count, step, 0, unroll=math.gcd(count, unroll))


def aligned(value, step):
    return pl.multiple_of(value, step)


AXES = ("gz", "gx", "gy")


def lane_index(rows):
    return lax.broadcasted_iota(jnp.int32, (rows, LANES), 1)


def parity(k):
    return lax.axis_index("gx") % 2 == k


class Exchange:
    def __init__(self, plan, number, refs, ends):
        self.plan, self.number, self.ends = plan, number, ends
        self.block, self.side, self.left, self.right, self.pack, self.send, self.recv = refs

    def copy(self, source, target, slot, place):
        return pltpu.make_async_remote_copy(
            src_ref=source,
            dst_ref=target,
            send_sem=self.send.at[self.number, slot],
            recv_sem=self.recv.at[self.number, slot],
            device_id=place,
            device_id_type=pl.DeviceIdType.MESH,
        )

    def pair(self, axis, source, targets, slot, guard=None, near=False):
        low, high = self.ends[axis]
        out = []
        for k, step in ((0, 1), (1, -1)):
            sends, receives = (high, low) if step == 1 else (low, high)
            if guard is not None:
                sends, receives = jnp.logical_and(sends, guard), jnp.logical_and(receives, guard)
            if near:
                sends, receives = jnp.logical_and(sends, parity(k)), jnp.logical_and(receives, parity(1 - k))
            out.append((sends, receives, self.copy(source, targets[k], slot + k, {axis: lax.axis_index(axis) + step})))
        return out

    def strips(self, spot, turn, slot):
        e, out = self.number, []
        low, high = self.ends["gy"]
        for k, step, target in ((0, 1, self.left), (1, -1, self.right)):
            sends, receives = (high, low) if step == 1 else (low, high)
            place = {"gy": lax.axis_index("gy") + step}
            if turn is not None:
                axis, shift = turn
                below, above = self.ends[axis]
                leaves, comes = (above, below) if shift == 1 else (below, above)
                if axis == "gx":
                    leaves = jnp.logical_and(leaves, parity(1 if shift == 1 else 0))
                    comes = jnp.logical_and(comes, parity(0 if shift == 1 else 1))
                sends, receives = jnp.logical_and(sends, leaves), jnp.logical_and(receives, comes)
                place[axis] = lax.axis_index(axis) + shift
            out.append((sends, receives, self.copy(self.pack.at[e, k], target.at[e, spot], slot + k, place)))
        return out

    def plans(self, brick):
        e, block, side = self.number, self.block, self.side
        low, high = self.ends["gz"]
        span = self.plan.rows // CHUNKS
        cuts = [pl.ds(c * span, span) for c in range(CHUNKS)]
        slots = iter(range(0, SLOTS, 2))
        self.y = self.strips(1, None, next(slots))
        self.x = self.pair("gx", brick, (block.at[e, 1, 0], block.at[e, 1, 2]), next(slots))
        self.side_z = [self.strips(0, ("gz", 1), next(slots)), self.strips(2, ("gz", -1), next(slots))]
        self.cross = [self.strips(3, ("gx", 1), next(slots)), self.strips(4, ("gx", -1), next(slots))]
        self.side_x = self.pair("gx", side.at[e, 1, 1], (side.at[e, 1, 0], side.at[e, 1, 2]), next(slots), None, True)
        self.z = [
            self.pair("gz", brick.at[cut], (block.at[e, 0, 1, cut], block.at[e, 2, 1, cut]), next(slots)) for cut in cuts
        ]
        self.far_x, self.far_side = [], []
        for zb, guard in ((0, low), (2, high)):
            self.far_x.append([
                self.pair("gx", block.at[e, zb, 1, cut], (block.at[e, zb, 0, cut], block.at[e, zb, 2, cut]), next(slots), guard)
                for cut in cuts
            ])
            self.far_side.append(
                self.pair("gx", side.at[e, zb, 1], (side.at[e, zb, 0], side.at[e, zb, 2]), next(slots), guard)
            )

    def begin(self, copies):
        for sends, _, item in copies:
            @pl.when(sends)
            def _(item=item):
                item.start()

    def arrive(self, copies):
        for _, receives, item in copies:
            @pl.when(receives)
            def _(item=item):
                item.wait_recv()

    def leave(self):
        far = [copies for both in self.far_x for copies in both]
        for copies in (self.y, self.x, *self.side_z, *self.cross, self.side_x, *self.z, *far, *self.far_side):
            for sends, _, item in copies:
                @pl.when(sends)
                def _(item=item):
                    item.wait_send()

    def start(self, brick):
        plan, e = self.plan, self.number
        self.plans(brick)
        self.begin(self.z[0])
        m, dense, width = plan.margin, plan.dense, plan.brick_y
        lane = lane_index(dense)
        head, tail = jnp.zeros((dense, LANES), F32), jnp.zeros((dense, LANES), F32)
        for j in range(LANES // m):
            rows = slice(j * dense, (j + 1) * dense)
            here = lane // m == j
            tail = jnp.where(here, pltpu.roll(brick[rows, width - LANES :], (j * m + m) % LANES, 1), tail)
            head = jnp.where(here, pltpu.roll(brick[rows, :LANES], j * m, 1) if j else brick[rows, :LANES], head)
        self.pack[e, 0] = tail
        self.pack[e, 1] = head
        self.begin(self.y)
        for copies in (*self.side_z, *self.cross):
            self.begin(copies)
        for copies in self.z[1:]:
            self.begin(copies)
        self.begin(self.x)

    def join(self, spot, zb, xb):
        m, e = self.plan.margin, self.number
        left, right = self.left[e, spot], self.right[e, spot]
        even = lane_index(self.plan.dense) // m % 2 == 0
        upper = jnp.where(even, left, pltpu.roll(right, m, 1))
        lower = jnp.where(even, pltpu.roll(left, LANES - m, 1), right)
        self.side[e, zb, xb] = jnp.concatenate([upper, lower], axis=0)

    def middle(self):
        self.arrive(self.y)
        self.join(1, 1, 1)
        self.begin(self.side_x)

    def forward(self, c):
        for k in range(2):
            self.arrive(self.z[c][k : k + 1])
            self.begin(self.far_x[k][c])

    def last(self):
        for k in range(2):
            @pl.when(self.ends["gz"][k])
            def _(k=k):
                self.arrive(self.side_z[k])
                self.join(2 * k, 2 * k, 1)
            self.begin(self.far_side[k])

    def row(self):
        self.arrive(self.x)
        self.arrive(self.side_x)
        for k in range(2):
            @pl.when(jnp.logical_and(self.ends["gx"][k], parity(k)))
            def _(k=k):
                self.arrive(self.cross[k])
                self.join(3 + k, 1, 2 * k)

    def far(self, k):
        for copies in self.far_x[k]:
            self.arrive(copies)
        self.arrive(self.far_side[k])


def psf_first(plan, p_ref, wy_ref, tz_ref, y_ref, sre_ref, sim_ref):
    extent = plan.extent
    total = jnp.sum(jnp.sum(p_ref[...], axis=0, keepdims=True), axis=1, keepdims=True)
    tiles = extent // plan.groups
    values = jnp.concatenate([p_ref[:, t * LANES : (t + 1) * LANES] for t in range(tiles)], axis=0)
    lane = lane_index(values.shape[0])
    for j in range(plan.groups):
        high, low = split(jnp.where(lane // extent == j, values, 0.0))
        out = dot(jnp.concatenate([high, low], axis=1), wy_ref[: 2 * LANES, :]) + dot(high, wy_ref[2 * LANES :, :])
        out = out / total
        for t in range(tiles):
            a = plan.groups * t + j
            y_ref[a * extent : (a + 1) * extent, :] = out[t * extent : (t + 1) * extent]

    def along_z(a):
        re, im = apply_left(tz_ref[...], y_ref[pl.ds(aligned(a * extent, 8), extent), :], -1)
        sre_ref[pl.ds(a, plan.length_z, stride=plan.pitch_psf), :] = re
        sim_ref[pl.ds(a, plan.length_z, stride=plan.pitch_psf), :] = im

    loop(extent, along_z, UNROLL)


def psf_second(plan, part, tx_ref, sre_ref, sim_ref, kre_ref, kim_ref):
    first = part * plan.length_z // PARTS
    count = (part + 1) * plan.length_z // PARTS - first

    def along_x(i):
        l = first + i
        rows = pl.ds(aligned(l * plan.pitch_psf, 8), plan.extent)
        values = jnp.concatenate([sre_ref[rows, :], sim_ref[rows, :]], axis=1)
        re, im = apply_left(tx_ref[...], values, -1)
        kre_ref[pl.ds(l, plan.length_x, stride=plan.pitch), :] = re
        kim_ref[pl.ds(l, plan.length_x, stride=plan.pitch), :] = im

    loop(count, along_x, UNROLL)


def block_y(plan, values, packed, wy_ref):
    core2, wide = 2 * plan.brick_y, plan.brick_y + LANES
    core_high, core_low = split(values)
    lane = lane_index(plan.packed)
    side = jnp.concatenate([jnp.where(lane // plan.extent == j, packed, 0.0) for j in range(plan.groups)], axis=0)
    side_high, side_low = split(side)
    return (
        dot(jnp.concatenate([core_high, core_low], axis=1), wy_ref[:core2, :])
        + dot(jnp.concatenate([core_high, side_high], axis=1), wy_ref[core2 : core2 + wide, :])
        + dot(jnp.concatenate([side_low, side_high], axis=1), wy_ref[core2 + wide :, :])
    )


def along_rows(plan, zb, tx_ref, scratch):
    y_ref, sre_ref, sim_ref = scratch[:3]
    bz, bx = plan.brick_z, plan.brick_x

    def along_x(z):
        rows = pl.ds(aligned(z * bx, 8), bx)
        values = jnp.concatenate([y_ref[zb, xb, rows, :] for xb in range(3)], axis=0)
        re, im = apply_left(tx_ref[...], values, -1)
        sre_ref[pl.ds(zb * bz + z, plan.length_x, stride=plan.pitch), :] = re
        sim_ref[pl.ds(zb * bz + z, plan.length_x, stride=plan.pitch), :] = im

    loop(bz, along_x, UNROLL)


def transform(plan, conj, tables, spectrum, scratch):
    tz_ref, bz_ref, bx_ref, by_ref = tables
    kre_ref, kim_ref = spectrum
    sre_ref, sim_ref, ire_ref, iim_ref, f_ref, q_ref = scratch[1:]
    length_z, length_x, pitch, back = plan.length_z, plan.length_x, plan.pitch, plan.pitch_back
    bz, bx, lanes = plan.brick_z, plan.brick_x, plan.lanes
    group = math.gcd(length_x, UNROLL)

    def along_z(step, i):
        k = step * group + i
        rows = pl.ds(aligned(k * pitch, 8), length_z)
        values = jnp.concatenate([sre_ref[rows, :], sim_ref[rows, :]], axis=1)
        re, im = apply_left(tz_ref[...], values, -1)
        kre, kim = kre_ref[rows, :], kim_ref[rows, :]
        if conj:
            pre, pim = re * kre + im * kim, im * kre - re * kim
        else:
            pre, pim = re * kre - im * kim, re * kim + im * kre
        high, low = split(jnp.concatenate([pre, pim], axis=1))
        q_ref[step % 2, i, :length_z] = high
        q_ref[step % 2, i, length_z:] = low

    def back_z(step, i):
        pair = q_ref[step % 2, i]
        out = dot(bz_ref[...], jnp.concatenate([pair, pair[:length_z]], axis=0))
        k = step * group + i
        ire_ref[pl.ds(k, bz, stride=back), :] = out[:bz, :lanes] - out[bz:, lanes:]
        iim_ref[pl.ds(k, bz, stride=back), :] = out[:bz, lanes:] + out[bz:, :lanes]

    steps = length_x // group
    for i in range(group):
        along_z(0, i)

    for step in range(steps - 1):
        for i in range(group):
            along_z(step + 1, i)
            back_z(step, i)

    for i in range(group):
        back_z(steps - 1, i)

    def back_x(z):
        rows = pl.ds(aligned(z * back, 8), length_x)
        values = jnp.concatenate([ire_ref[rows, :], iim_ref[rows, :]], axis=1)
        re, im = apply_left(bx_ref[...], values, 1)
        f_ref[pl.ds(aligned(z * bx, 8), bx), :] = jnp.concatenate([re, im], axis=1)

    loop(bz, back_x, UNROLL)
    high, low = split(f_ref[...])
    by = plan.brick_y
    both = dot(high, by_ref[...])
    return both[:, :by] + both[:, by:] + dot(low, by_ref[:, :by])


def kernel(plan, *rest):
    sources = rest[:12]
    out_ref, across_ref, along_ref, top_ref = rest[12:16]
    held = rest[16:28]
    e_ref, m_ref, p_ref, psf_y, psf_x, psf_z, wy_ref = held[:7]
    tables = held[7:]
    (block, side, left, right, pack, ratio, py_ref, pre_ref, pim_ref, kre_ref, kim_ref,
     y_ref, sre_ref, sim_ref, ire_ref, iim_ref, f_ref, q_ref,
     most_z, most_x, most_y, send, recv, most_send, most_recv, fetch) = rest[28:]
    most = {"gz": most_z, "gx": most_x, "gy": most_y}
    count = plan.mesh

    ends = {axis: (lax.axis_index(axis) > 0, lax.axis_index(axis) < count[axis] - 1) for axis in AXES}
    barrier = pltpu.get_barrier_semaphore()
    greet = []
    for axis in AXES:
        if max(count[axis] for axis in AXES) <= NEAR:
            for k, d in enumerate((-1, 1)):
                greet.append((ends[axis][k], {axis: lax.axis_index(axis) + d}))
        else:
            for d in range(1, count[axis]):
                greet.append((None, {axis: (lax.axis_index(axis) + d) % count[axis]}))
    for axis in ("gz", "gx"):
        for k, d in enumerate((-1, 1)):
            for n, step in enumerate((-1, 1)):
                place = {axis: lax.axis_index(axis) + d, "gy": lax.axis_index("gy") + step}
                greet.append((jnp.logical_and(ends[axis][k], ends["gy"][n]), place))
    total = 0
    for has, place in greet:
        def signal(place=place):
            pl.semaphore_signal(barrier, inc=1, device_id=place, device_id_type=pl.DeviceIdType.MESH)

        if has is None:
            signal()
            total = total + 1
        else:
            pl.when(has)(signal)
            total = total + has.astype(jnp.int32)
    fetched = [pltpu.make_async_copy(sources[i], held[i], fetch.at[i]) for i in range(12)]
    for i in (0, 2, 3, 5, 4, 6, 1, 7, 8, 9, 10, 11):
        fetched[i].start()
    pl.semaphore_wait(barrier, total)

    valid_z = (ends["gz"][0], ends["gz"][0] | True, ends["gz"][1])
    valid_x = (ends["gx"][0], ends["gx"][0] | True, ends["gx"][1])
    refs = (block, side, left, right, pack, send, recv)
    first, second = Exchange(plan, 0, refs, ends), Exchange(plan, 1, refs, ends)

    fetched[0].wait()
    first.start(e_ref)
    for target, has in ((left, ends["gy"][0]), (right, ends["gy"][1])):
        @pl.when(jnp.logical_not(has))
        def _(target=target):
            target[...] = jnp.zeros_like(target)
    for zb in (0, 2):
        @pl.when(jnp.logical_not(valid_z[zb]))
        def _(zb=zb):
            def clear(k):
                rows = pl.ds(aligned(k * plan.pitch + zb * plan.brick_z, 8), plan.brick_z)
                zero = jnp.zeros((plan.brick_z, plan.lanes), F32)
                sre_ref[rows, :] = zero
                sim_ref[rows, :] = zero

            loop(plan.length_x, clear, 8)
    for xb in (0, 2):
        @pl.when(jnp.logical_not(valid_x[xb]))
        def _(xb=xb):
            for e in range(2):
                for zb in range(3):
                    block[e, zb, xb] = jnp.zeros((plan.rows, plan.brick_y), F32)
                    side[e, zb, xb] = jnp.zeros((plan.packed, LANES), F32)

    def along_y(exchange, zb, spots, brick):
        @pl.when(valid_z[zb])
        def _():
            e = exchange.number
            for xb in spots:
                values = brick[...] if (zb, xb) == (1, 1) else block[e, zb, xb]
                y_ref[zb, xb] = block_y(plan, values, side[e, zb, xb], wy_ref)

    scratch = (y_ref, sre_ref, sim_ref, ire_ref, iim_ref, f_ref, q_ref)
    tx_ref = tables[0]

    def rows_of(zb):
        @pl.when(valid_z[zb])
        def _():
            along_rows(plan, zb, tx_ref, scratch)

    def own(exchange, brick):
        along_y(exchange, 1, (1,), brick)

    def sides(exchange, brick):
        exchange.row()
        along_y(exchange, 1, (0, 2), brick)

    def above(exchange, brick):
        along_y(exchange, 0, (1,), brick)
        along_y(exchange, 2, (1,), brick)

    def corners(exchange, brick):
        for k, zb in enumerate((0, 2)):
            exchange.far(k)
            along_y(exchange, zb, (0, 2), brick)
            rows_of(zb)

    for i in (2, 3, 5):
        fetched[i].wait()
    psf_first(plan, p_ref, psf_y, psf_z, py_ref, pre_ref, pim_ref)
    fetched[4].wait()
    psf_second(plan, 0, psf_x, pre_ref, pim_ref, kre_ref, kim_ref)
    psf_second(plan, 1, psf_x, pre_ref, pim_ref, kre_ref, kim_ref)
    psf_second(plan, 2, psf_x, pre_ref, pim_ref, kre_ref, kim_ref)
    first.middle()
    first.forward(0)
    first.last()
    first.forward(1)
    for i in (6, 1, 7, 8, 9, 10, 11):
        fetched[i].wait()
    own(first, e_ref)
    sides(first, e_ref)
    rows_of(1)
    above(first, e_ref)
    corners(first, e_ref)
    blurred = transform(plan, False, tables[1:], (kre_ref, kim_ref), scratch)
    ratio[...] = m_ref[...] / blurred

    second.start(ratio)
    second.middle()
    second.forward(0)
    second.last()
    second.forward(1)
    own(second, ratio)
    sides(second, ratio)
    rows_of(1)
    above(second, ratio)
    corners(second, ratio)
    correction = transform(plan, True, tables[1:], (kre_ref, kim_ref), scratch)
    updated = (e_ref[...] * correction).reshape(plan.brick_z, plan.brick_x, plan.brick_y)

    copies = {}
    slot = 0

    def share(axis):
        nonlocal slot
        copies[axis] = []
        for d in range(count[axis] - 1, 0, -1):
            item = pltpu.make_async_remote_copy(
                src_ref=most[axis].at[0],
                dst_ref=most[axis].at[d],
                send_sem=most_send.at[slot],
                recv_sem=most_recv.at[slot],
                device_id={axis: (lax.axis_index(axis) + d) % count[axis]},
                device_id_type=pl.DeviceIdType.MESH,
            )
            item.start()
            copies[axis].append((d, item))
            slot += 1

    most_y[0] = jnp.zeros((plan.brick_z, LANES), F32)
    most_y[0, :, : plan.brick_x] = jnp.max(updated, axis=2)
    share("gy")
    most_x[0] = jnp.max(updated, axis=1)
    share("gx")
    most_z[0] = jnp.max(updated, axis=0)
    share("gz")
    out_ref[...] = updated
    first.leave()
    second.leave()
    found = {}
    for axis in AXES:
        value = most[axis][0]
        for d, item in copies[axis]:
            item.wait_recv()
            value = jnp.maximum(value, most[axis][d])
        found[axis] = value
    across_ref[...] = found["gx"]
    along_ref[...] = found["gy"][:, : plan.brick_x]
    piece = plan.brick_y // count["gz"]
    for i in range(count["gz"]):
        @pl.when(lax.axis_index("gz") == i)
        def _(i=i):
            top_ref[...] = found["gz"][:, i * piece : (i + 1) * piece]
    for axis in AXES:
        for _, item in copies[axis]:
            item.wait_send()


def deliver(count, *refs):
    sources, targets, sems = refs[:count], refs[count : 2 * count], refs[-1]
    outward = [pltpu.make_async_copy(sources[i], targets[i], sems.at[i]) for i in range(count)]
    for item in outward:
        item.start()
    for item in outward:
        item.wait()


def shards(sizes, estimate, measured, point_spread):
    plan = Plan(estimate.shape, point_spread.shape[0], sizes)
    bz, bx, by, rows = plan.brick_z, plan.brick_x, plan.brick_y, plan.rows
    args = (estimate.reshape(rows, by), measured.reshape(rows, by), point_spread, *plan.tables())
    vmem = pl.BlockSpec(memory_space=pltpu.VMEM)
    outs = [(bz, bx, by), (bz, by), (bz, bx), (bx, by // sizes["gz"])]
    spread = (plan.length_x * plan.pitch, plan.lanes)
    psf_spread = (plan.length_z * plan.pitch_psf, plan.lanes)
    back = (bz * plan.pitch_back, plan.lanes)
    shapes = [
        (2, 3, 3, rows, by), (2, 3, 3, plan.packed, LANES), (2, 5, plan.dense, LANES), (2, 5, plan.dense, LANES),
        (2, 2, plan.dense, LANES), (rows, by), (plan.extent * plan.extent, 2 * plan.lanes), psf_spread, psf_spread,
        spread, spread, (3, 3, rows, 2 * plan.lanes), spread, spread, back, back, (rows, 2 * plan.lanes),
        (sizes["gz"], bx, by), (sizes["gx"], bz, by), (sizes["gy"], bz, LANES),
    ]
    peers = sum(sizes[axis] - 1 for axis in AXES)
    sems = pltpu.SemaphoreType.DMA
    held = [pltpu.VMEM(item.shape, item.dtype) for item in args]
    queue = (2, math.gcd(plan.length_x, UNROLL), 2 * plan.length_z, 2 * plan.lanes)
    scratch = [pltpu.VMEM(shape, F32) for shape in shapes]
    scratch.insert(17, pltpu.VMEM(queue, BF16))
    results = pl.pallas_call(
        functools.partial(kernel, plan),
        out_shape=[pltpu.VMEM(shape, F32) for shape in outs],
        in_specs=[pl.BlockSpec(memory_space=pltpu.HBM)] * len(args),
        out_specs=[vmem] * len(outs),
        scratch_shapes=held + scratch
        + [sems((2, SLOTS)), sems((2, SLOTS)), sems((peers,)), sems((peers,)), sems((len(args),))],
        compiler_params=pltpu.CompilerParams(collective_id=0, has_side_effects=True, vmem_limit_bytes=GRANT),
    )(*args)
    return pl.pallas_call(
        functools.partial(deliver, len(outs)),
        out_shape=[jax.ShapeDtypeStruct(shape, F32) for shape in outs],
        in_specs=[vmem] * len(outs),
        out_specs=[pl.BlockSpec(memory_space=pltpu.HBM)] * len(outs),
        scratch_shapes=[sems((len(outs),))],
        compiler_params=pltpu.CompilerParams(vmem_limit_bytes=ROOM),
    )(*results)


def solution(mesh):
    in_specs = (P("gz", "gx", "gy"), P("gz", "gx", "gy"), P())
    out_specs = (P("gz", "gx", "gy"), P("gz", "gy"), P("gz", "gx"), P("gx", ("gy", "gz")))
    body = functools.partial(shards, {axis: mesh.shape[axis] for axis in AXES})
    return jax.shard_map(lambda *args: tuple(body(*args)), mesh=mesh, in_specs=in_specs, out_specs=out_specs, check_vma=False)
```
